512 devices in a mesh: dp: 32 (over y, z_lo, core), mp: 16 (over x, z_hi).
Axes of the slice: x: 4, y: 4, z: 16 (z_hi: 4, z_lo: 4; z = z_hi * 4 + z_lo), core: 2. Of those that a mesh axis runs over, the one named last changes fastest.
Arguments:
- token_ids: int32 [64], replicated, may hold values from 0 to 49151
- cache_lengths: int32 [64], P('dp'), may hold values from 1 to 512
- embedding: bfloat16 [49152, 12288], P(('dp', 'mp')), may hold values from -6 to 6
- ln_gain: float32 [12288], replicated, may hold values from 0.25 to 1.75
- query_weight: bfloat16 [12288, 6144], P('dp', 'mp'), may hold values from -0.0546875 to 0.0546875
- key_cache: bfloat16 [64, 512, 6144], P('dp', None, 'mp'), may hold values from -1000 to 1000
- value_cache: bfloat16 [64, 512, 6144], P('dp', None, 'mp'), may hold values from -6 to 6
- out_weight: bfloat16 [6144, 12288], P('mp', 'dp'), may hold values from -0.078125 to 0.078125
- final_gain: float32 [12288], replicated, may hold values from 0.25 to 1.75
Outputs:
- log_probs: float32 [64, 49152], P(None, ('dp', 'mp'))
The draws below stay inside these ranges and needn't reach their ends.
All inputs are finite; a program needn't handle non-finite values.
Results may differ from the reference program's by a relative error of at most 0.00033.
Values may be sent and summed in bfloat16 or wider, within the bound.
A program may use at most 64 MiB of HBM per device.

```python
import math
import jax
import jax.numpy as jnp
import numpy as np
from jax import lax

D = 12288
HEADS = 48
HD = 128
CACHE = 512
HQ = 6144
SEQS = 64
VOCAB = 49152


def draw_key_cache(key, part):
    noise_key, dir_key, str_key, pick_key, pos_key = jax.random.split(jax.random.fold_in(key, 7), 5)
    base_noise = jnp.clip(jax.random.normal(noise_key, (SEQS, CACHE, HQ), jnp.float32), -6.0, 6.0)
    lowest = 100.0
    highest = 180.0
    share_of = 0.5
    direction = jnp.clip(jax.random.normal(dir_key, (SEQS, HQ), jnp.float32), -3.0, 3.0)
    strength = lowest * (highest / lowest) ** jax.random.uniform(str_key, (SEQS,), jnp.float32)
    chosen = (jax.random.uniform(pick_key, (SEQS,), jnp.float32) < share_of).astype(jnp.float32)
    position = jax.random.randint(pos_key, (SEQS,), 0, CACHE // 4)
    slot_index = jnp.arange(CACHE)[None, :]
    at_first = (slot_index == position[:, None])[:, :, None]
    at_second = (slot_index == position[:, None] + 1)[:, :, None]
    first_row = jnp.sum(jnp.where(at_first, base_noise, 0.0), axis=1) + (chosen * strength)[:, None] * direction
    planted = jnp.where(at_first, first_row[:, None, :], base_noise)
    planted = jnp.where(at_second, (1.012 * first_row)[:, None, :], planted)
    return planted.astype(jnp.bfloat16)


def set_ends(values, key, least, largest):
    index_at = [jax.random.randint(jax.random.fold_in(key, axis), (), 0, length) for axis, length in enumerate(values.shape)]
    longest = values.shape.index(max(values.shape))
    next_to = index_at[:longest] + [(index_at[longest] + 1) % values.shape[longest]] + index_at[longest + 1:]
    return values.at[tuple(index_at)].set(least).at[tuple(next_to)].set(largest)


def block_scale(stream_key, shape, pieces, smallest, high):
    level, own = 1.0, jax.random.fold_in(stream_key, 6)
    for dim, blocks in pieces:
        steps = jnp.exp(jax.random.uniform(jax.random.fold_in(own, dim), (blocks,), jnp.float32, smallest / len(pieces), high / len(pieces)))
        level = level * jnp.repeat(steps, shape[dim] // blocks).reshape([-1 if axis == dim else 1 for axis in range(len(shape))])
    return level


def cumulative_ranks(amount, skew):
    portions = [(1 << 20) // math.isqrt(rank ** skew) + 1 for rank in range(1, amount + 1)]
    spread = 1 + sum(portions) // (1 << 30)
    return np.cumsum(np.array([max(1, weight // spread) for weight in portions]))


def ranked_ids(rng, dims, amount, slope):
    listing = cumulative_ranks(amount, slope)
    ticket = jax.random.randint(jax.random.fold_in(rng, 1), dims, 0, int(listing[amount - 1]))
    grade = jnp.searchsorted(jnp.asarray(listing, jnp.int32), ticket, side="right")
    return jax.random.permutation(jax.random.fold_in(rng, 2), amount)[grade].astype(jnp.int32)


def normal_values(rng, extent, width, bound, shards=(), kind=jnp.bfloat16):
    drawn = width * jax.random.normal(rng, extent, jnp.float32)
    if shards:
        drawn = drawn * block_scale(rng, extent, shards, -0.22, 0.18)
    return jnp.clip(drawn, -bound, bound).astype(kind)


def setup_inputs(seed: int = 0) -> dict:
    seeds = jax.random.split(jax.random.key(seed), 10)
    token_ids = set_ends(ranked_ids(seeds[0], (SEQS,), VOCAB, 2), jax.random.fold_in(seeds[0], 3), 0, VOCAB - 1).astype(jnp.int32)
    cache_lengths = set_ends(jax.random.randint(seeds[1], (SEQS,), 1, CACHE + 1), jax.random.fold_in(seeds[1], 1), 1, CACHE).astype(jnp.int32)
    embedding = normal_values(seeds[2], (VOCAB, D), 1.0, 6.0, ((0, 512),))
    ln_gain = jnp.clip(1.0 + 0.15 * jax.random.normal(seeds[3], (D,), jnp.float32), 0.25, 1.75)
    query_weight = normal_values(seeds[4], (D, HQ), D ** -0.5, 0.0546875, ((0, 32), (1, 16)))
    key_cache = draw_key_cache(jax.random.fold_in(seeds[9], 71), 0)
    value_cache = normal_values(seeds[6], (SEQS, CACHE, HQ), 1.0, 6.0, ((0, 32), (2, 16)))
    out_weight = normal_values(seeds[7], (HQ, D), HQ ** -0.5, 0.078125, ((0, 16), (1, 32)))
    final_gain = jnp.clip(1.0 + 0.15 * jax.random.normal(seeds[8], (D,), jnp.float32), 0.25, 1.75)
    return {"token_ids": token_ids, "cache_lengths": cache_lengths, "embedding": embedding, "ln_gain": ln_gain, "query_weight": query_weight, "key_cache": key_cache, "value_cache": value_cache, "out_weight": out_weight, "final_gain": final_gain}


def layer_norm(values_in, gain_vec):
    row_mean = lax.optimization_barrier(jnp.mean(values_in, axis=-1, keepdims=True))
    centred = values_in - row_mean
    row_var = lax.optimization_barrier(jnp.mean(centred * centred, axis=-1, keepdims=True))
    return gain_vec * centred * lax.rsqrt(row_var + 1e-05)

def reference(token_ids, cache_lengths, embedding, ln_gain, query_weight, key_cache, value_cache, out_weight, final_gain):
    embedded = embedding[token_ids].astype(jnp.float32)
    normed = layer_norm(embedded, ln_gain).astype(jnp.bfloat16)
    queries = (jnp.dot(normed, query_weight, preferred_element_type=jnp.float32) * HD ** (-0.5)).astype(jnp.bfloat16)

    def attend_one(operands):
        query_row, key_rows, value_rows, length = operands
        head_query = query_row.reshape(HEADS, HD).astype(jnp.float32)
        key_heads = key_rows.reshape(CACHE, HEADS, HD).astype(jnp.float32)
        value_heads = value_rows.reshape(CACHE, HEADS, HD).astype(jnp.float32)
        scores = jnp.einsum('hd,thd->ht', head_query, key_heads)
        live_mask = jnp.arange(CACHE).astype(jnp.int32) < length
        scores = jnp.where(live_mask[None, :], scores, jnp.float32(-1e+30))
        row_top = lax.optimization_barrier(jnp.max(scores, axis=-1, keepdims=True))
        exp_terms = jnp.exp(scores - row_top)
        weights = (exp_terms / lax.optimization_barrier(jnp.sum(exp_terms, axis=-1, keepdims=True))).astype(jnp.bfloat16)
        result = jnp.einsum('ht,thd->hd', weights.astype(jnp.float32), value_heads)
        return result.reshape(HQ).astype(jnp.bfloat16)
    attended = lax.map(attend_one, (queries, key_cache, value_cache, cache_lengths))
    hidden = embedded + jnp.dot(attended, out_weight, preferred_element_type=jnp.float32)
    final_normed = layer_norm(hidden, final_gain).astype(jnp.bfloat16)
    logits = jnp.dot(final_normed, embedding.T, preferred_element_type=jnp.float32)
    return jax.nn.log_softmax(logits, axis=-1)
```

```python
import functools

import jax
import jax.numpy as jnp
from jax import lax
from jax.experimental import pallas as pl
from jax.experimental.pallas import tpu as pltpu
from jax.sharding import Mesh
from jax.sharding import PartitionSpec as P

HD = 128
EPS = 1e-5
DP_MP = ("dp_0", "dp_1", "dp_2", "mp_0", "mp_1")
DP = ("dp_0", "dp_1", "dp_2")
MP = ("mp_0", "mp_1")
MESH = pl.DeviceIdType.MESH
F32 = jnp.float32
BF16 = jnp.bfloat16
NSEM = 20


def kernel(
    sizes,
    ids_ref, len_ref, emb_ref, lng_ref, wq_ref, key_ref, val_ref, wo_ref, fg_ref,
    out_ref,
    emb, wq, key, val, wo,
    p, r1, r2, a3, r3, r4, r5, s1, s2, s3, s4,
    part, rq, ra, att_all, op, ro1, ro2, rs, fb, g1, g2, g3,
    load_sem, send_sem, recv_sem,
):
    Y, Z, C, X, H = sizes
    NDP, XY, ZC = Y * Z * C, X * Y, Z * C
    V, D = emb.shape
    SP, T, HW = key.shape
    W = D // NDP
    SEQ = SP * NDP
    R = SEQ // X
    NH = HW // HD

    yi, zi, ci, xi, hi = (lax.axis_index(a) for a in DP_MP)
    xy = xi * Y + yi
    zc = zi * C + ci
    dp = (yi * Z + zi) * C + ci

    def xy_dev(i):
        return {"mp_0": lax.div(i, Y), "dp_0": lax.rem(i, Y)}

    def zc_dev(i):
        return {"dp_1": lax.div(i, C), "dp_2": lax.rem(i, C)}

    def dp_dev(i):
        return {"dp_0": lax.div(i, ZC), "dp_1": lax.rem(lax.div(i, C), Z), "dp_2": lax.rem(i, C)}

    def z_dev(i):
        return {"dp_1": i}

    def c_dev(i):
        return {"dp_2": i}

    def x_dev(i):
        return {"mp_0": i}

    def h_dev(i):
        return {"mp_1": i}

    def each(n, body):
        if n <= 4:
            for k in range(1, n):
                body(k)
        else:
            lax.fori_loop(1, n, lambda k, _: body(k), None)

    def send(s, src, dst, dev):
        pltpu.make_async_remote_copy(
            src_ref=src, dst_ref=dst, send_sem=send_sem.at[s], recv_sem=recv_sem.at[s],
            device_id=dev, device_id_type=MESH,
        ).start()

    def take(sem, ref):
        pltpu.make_async_copy(ref, ref, sem).wait()

    pending = []

    def arrived(s, ref):
        take(recv_sem.at[s], ref)
        pending.append((s, ref))

    def exchange(s, src, dst, own, n, dev):
        def body(k):
            i = lax.rem(own + k, n)
            send(s, src.at[i], dst.at[own], dev(i))

        each(n, body)

    def gather(s, buf, own, n, dev):
        def body(k):
            i = lax.rem(own + k, n)
            send(s, buf.at[own], buf.at[own], dev(i))

        each(n, body)

    def to_rows(cols):
        n = cols[0].shape[0]
        lane = lax.broadcasted_iota(jnp.int32, (n, 128), 1)
        x = jnp.zeros((n, 128), F32)
        for k, col in enumerate(cols):
            x = jnp.where(lane == k, col, x)
        if n < 128:
            x = jnp.concatenate([x, jnp.zeros((128 - n, 128), F32)], axis=0)
        return jnp.transpose(x)

    def to_cols(rows):
        row = lax.broadcasted_iota(jnp.int32, (128, 128), 0)
        x = jnp.zeros((128, 128), F32)
        for k, r in enumerate(rows):
            x = jnp.where(row == k, r, x)
        return jnp.transpose(x)

    loads = [
        pltpu.make_async_copy(a, b, load_sem.at[i])
        for i, (a, b) in enumerate(
            ((emb_ref, emb), (wq_ref, wq), (key_ref, key), (val_ref, val), (wo_ref, wo))
        )
    ]
    for c in loads:
        c.start()

    barrier = pltpu.get_barrier_semaphore()

    def greet(dev):
        pl.semaphore_signal(barrier, inc=1, device_id=dev, device_id_type=MESH)

    each(H, lambda k: greet(h_dev(lax.rem(hi + k, H))))
    each(NDP, lambda k: greet(dp_dev(lax.rem(dp + k, NDP))))
    for kx in range(1, X):
        for ky in range(Y):
            greet({"mp_0": lax.rem(xi + kx, X), "dp_0": lax.rem(yi + ky, Y)})

    flat = (dp * X + xi) * H + hi
    ids = ids_ref[...]
    if SEQ < 128:
        ids = jnp.concatenate([ids, jnp.full((1, 128 - SEQ), -1, jnp.int32)], axis=1)
    row = lax.broadcasted_iota(jnp.int32, (128, 128), 0)
    hot = jnp.where((row + flat * V == ids) & (row < V), 1.0, 0.0).astype(F32)
    hot = jnp.transpose(hot)[:SEQ, :V].astype(BF16)

    loads[0].wait()
    other = 1 - ci
    acc = jnp.zeros((SEQ, 128), F32)
    for half in (other, ci):
        for yy in range(Y):
            for zz in range(Z):
                b = (yy * Z + zz) * C + half
                cols = pl.ds(pl.multiple_of(b * W, 128), W)
                blk = jnp.dot(hot, emb[:, cols], preferred_element_type=F32)
                for j in range(0, W, 128):
                    acc = acc + blk[:, j : j + 128]
                blk = blk.astype(BF16)
                for xx in range(X):
                    p[half, xx * Y + yy, zz] = blk[xx * R : (xx + 1) * R]
        if half is other:
            pl.semaphore_wait(barrier, NDP - 1 + (X - 1) * Y + H - 1)
            send(0, p.at[other], r1, c_dev(other))
    mean = jnp.sum(acc, axis=1, keepdims=True) / D
    devs = []
    for xx in range(X):
        m = mean[xx * R : (xx + 1) * R]
        sq = jnp.zeros((R, 128), F32)
        for cc in range(C):
            for yy in range(Y):
                for zz in range(Z):
                    d = p[cc, xx * Y + yy, zz].astype(F32) - m
                    for j in range(0, W, 128):
                        sq = sq + d[:, j : j + 128] * d[:, j : j + 128]
        devs.append(jnp.sum(sq, axis=1, keepdims=True) / D)
    var = jnp.concatenate(devs, axis=0)
    s1[ci] = to_rows((mean, var))[:8]
    gather(1, s1, ci, C, c_dev)

    arrived(0, r1)
    for k in range(XY):
        r1[k] = r1[k] + p[ci, k]
    exchange(2, r1, r2, xy, XY, xy_dev)
    r2[xy] = r1[xy]
    arrived(1, s1.at[pl.ds(0, C - 1)])
    s2[xy] = jnp.sum(s1[...], axis=0)
    gather(3, s2, xy, XY, xy_dev)

    arrived(2, r2.at[pl.ds(0, XY - 1)])
    for zz in range(Z):
        tot = r2[0, zz]
        for k in range(1, XY):
            tot = tot + r2[k, zz]
        a3[zz] = tot
    exchange(4, a3, r3, zi, Z, z_dev)
    r3[zi] = a3[zi]
    arrived(3, s2.at[pl.ds(0, XY - 1)])
    s3[zi] = jnp.sum(s2[...], axis=0)
    gather(5, s3, zi, Z, z_dev)

    arrived(4, r3.at[pl.ds(0, Z - 1)])
    tot = r3[0]
    for k in range(1, Z):
        tot = tot + r3[k]
    r4[hi] = tot
    if H > 1:
        gather(6, r4, hi, H, h_dev)
    arrived(5, s3.at[pl.ds(0, Z - 1)])
    s4[hi] = jnp.sum(s3[...], axis=0)
    if H > 1:
        gather(7, s4, hi, H, h_dev)

        arrived(6, r4.at[pl.ds(0, H - 1)])
    tot = r4[0]
    for k in range(1, H):
        tot = tot + r4[k]
    r5[xi] = tot
    gather(8, r5, xi, X, x_dev)
    if H > 1:
        arrived(7, s4.at[pl.ds(0, H - 1)])
    stats = jnp.sum(s4[...], axis=0)
    stats = to_cols((stats[0:1], stats[1:2]))
    mean, var = stats[:SEQ, 0:1], stats[:SEQ, 1:2]
    arrived(8, r5.at[pl.ds(0, X - 1)])

    own_cols = pl.ds(pl.multiple_of(dp * W, 128), W)
    embedded = r5[...].reshape(SEQ, W).astype(F32)
    normed = (lng_ref[:, own_cols] * (embedded - mean) * lax.rsqrt(var + EPS)).astype(BF16)
    loads[1].wait()
    partial = jnp.dot(normed, wq[...], preferred_element_type=F32)
    for j in range(NDP):
        part[j] = partial[j * SP : (j + 1) * SP]
    exchange(9, part, rq, dp, NDP, dp_dev)
    rq[dp] = part[dp]
    loads[2].wait()
    loads[3].wait()
    arrived(9, rq.at[pl.ds(0, NDP - 1)])
    queries = (jnp.sum(rq[...], axis=0) * HD**-0.5).astype(BF16).astype(F32)

    head = lax.broadcasted_iota(jnp.int32, (8, HW), 0) * HD
    lane = lax.broadcasted_iota(jnp.int32, (8, HW), 1)
    own_head = (lane >= head) & (lane < head + HD)
    place = lax.broadcasted_iota(jnp.int32, (8, T), 1)
    pair = lax.broadcasted_iota(jnp.int32, (SP, HW), 0)
    attended = jnp.zeros((SP, HW), F32)
    for s in range(SP):
        q = jnp.where(own_head, queries[s : s + 1], 0.0).astype(BF16)
        scores = lax.dot_general(
            q, key[s], (((1,), (1,)), ((), ())), preferred_element_type=F32
        )
        scores = jnp.where(place < len_ref[s], scores, -1e30)
        e = jnp.exp(scores - jnp.max(scores, axis=1, keepdims=True))
        w = (e / jnp.sum(e, axis=1, keepdims=True)).astype(BF16)
        got = jnp.dot(w, val[s], preferred_element_type=F32)
        got = jnp.sum(jnp.where(own_head, got, 0.0), axis=0, keepdims=True)
        attended = jnp.where(pair == s, got, attended)
    ra[dp] = attended.astype(BF16).astype(F32)
    gather(10, ra, dp, NDP, dp_dev)
    loads[4].wait()
    arrived(10, ra.at[pl.ds(0, NDP - 1)])
    for j in range(NDP):
        att_all[j * SP : (j + 1) * SP] = ra[j]

    mixed = jnp.dot(att_all[...].astype(BF16), wo[...], preferred_element_type=F32)
    for xx in range(X):
        op[xx] = mixed[xx * R : (xx + 1) * R]
    exchange(11, op, ro1, xi, X, x_dev)
    ro1[xi] = op[xi]
    arrived(11, ro1.at[pl.ds(0, X - 1)])
    ro2[hi] = jnp.sum(ro1[...], axis=0)
    if H > 1:
        gather(12, ro2, hi, H, h_dev)
        arrived(12, ro2.at[pl.ds(0, H - 1)])
    hidden = r5[xi].astype(F32) + jnp.sum(ro2[...], axis=0)

    m = jnp.sum(hidden, axis=1, keepdims=True) / W
    d = hidden - m
    rs[dp] = to_rows((m, jnp.sum(d * d, axis=1, keepdims=True)))[:2]
    gather(13, rs, dp, NDP, dp_dev)
    arrived(13, rs.at[pl.ds(0, NDP - 1)])
    blocks = rs[...]
    row_mean = jnp.sum(blocks, axis=0)[0:1] / NDP
    off = blocks[:, 0:1] - row_mean[None]
    row_var = jnp.sum(blocks[:, 1:2] + W * (off * off), axis=0) / D
    stats = to_cols((row_mean, lax.rsqrt(row_var + EPS)))
    fn = fg_ref[:, own_cols] * (hidden - stats[:R, 0:1]) * stats[:R, 1:2]
    fb[ci, xy, zi] = fn.astype(BF16)

    def f1(k):
        z = lax.rem(zi + k, Z)
        send(14, fb.at[ci, xy, zi], fb.at[ci, xy, zi], z_dev(z))

    each(Z, f1)
    arrived(14, fb.at[ci, xy, pl.ds(0, Z - 1)])

    def f2(k):
        i = lax.rem(xy + k, XY)
        send(15, fb.at[ci, xy], fb.at[ci, xy], xy_dev(i))

    each(XY, f2)
    arrived(15, fb.at[ci, pl.ds(0, XY - 1)])
    send(16, fb.at[ci], fb.at[ci], c_dev(other))
    arrived(16, fb.at[other])

    logits = jnp.zeros((SEQ, V), F32)
    for yy in range(Y):
        for zz in range(Z):
            lhs = jnp.concatenate(
                [
                    jnp.concatenate([fb[cc, xx * Y + yy, zz] for xx in range(X)], axis=0)
                    for cc in range(C)
                ],
                axis=1,
            )
            b = (yy * Z + zz) * C * W
            logits = logits + lax.dot_general(
                lhs, emb[:, b : b + C * W], (((1,), (1,)), ((), ())), preferred_element_type=F32
            )
    top = jnp.max(logits, axis=1, keepdims=True)
    total = jnp.sum(jnp.exp(logits - top), axis=1, keepdims=True)
    slab = to_rows((top, total))[:2]

    def merged(buf):
        v = buf[...]
        tops, sums = v[:, 0:1], v[:, 1:2]
        best = jnp.max(tops, axis=0)
        return best, jnp.sum(sums * jnp.exp(tops - best[None]), axis=0)

    def joined(best, tot):
        r = lax.broadcasted_iota(jnp.int32, (2, 128), 0)
        return jnp.where(r == 0, best, tot)

    g1[xy] = slab
    gather(17, g1, xy, XY, xy_dev)
    arrived(17, g1.at[pl.ds(0, XY - 1)])
    g2[zc] = joined(*merged(g1))
    gather(18, g2, zc, ZC, zc_dev)
    arrived(18, g2.at[pl.ds(0, ZC - 1)])
    g3[hi] = joined(*merged(g2))
    if H > 1:
        gather(19, g3, hi, H, h_dev)
        arrived(19, g3.at[pl.ds(0, H - 1)])
    best, tot = merged(g3)
    stats = to_cols((best, jnp.log(tot)))
    out_ref[...] = (logits - stats[:SEQ, 0:1]) - stats[:SEQ, 1:2]
    for s, ref in pending:
        take(send_sem.at[s], ref)


def per_device(sizes, token_ids, cache_lengths, embedding, ln_gain, query_weight, key_cache,
               value_cache, out_weight, final_gain):
    Y, Z, C, X, H = sizes
    NDP, XY = Y * Z * C, X * Y
    V, D = embedding.shape
    SP, T, HW = key_cache.shape
    W = D // NDP
    SEQ = SP * NDP
    R = SEQ // X
    vmem = pl.BlockSpec(memory_space=pltpu.VMEM)
    smem = pl.BlockSpec(memory_space=pltpu.SMEM)
    hbm = pl.BlockSpec(memory_space=pl.ANY)
    return pl.pallas_call(
        functools.partial(kernel, sizes),
        name="decode",
        out_shape=jax.ShapeDtypeStruct((SEQ, V), F32),
        in_specs=[vmem, smem, hbm, vmem, hbm, hbm, hbm, hbm, vmem],
        out_specs=vmem,
        scratch_shapes=[
            pltpu.VMEM((V, D), BF16),
            pltpu.VMEM((W, HW), BF16),
            pltpu.VMEM((SP, T, HW), BF16),
            pltpu.VMEM((SP, T, HW), BF16),
            pltpu.VMEM((HW, W), BF16),
            pltpu.VMEM((C, XY, Z, R, W), BF16),
            pltpu.VMEM((XY, Z, R, W), BF16),
            pltpu.VMEM((XY, Z, R, W), BF16),
            pltpu.VMEM((Z, R, W), BF16),
            pltpu.VMEM((Z, R, W), BF16),
            pltpu.VMEM((H, R, W), BF16),
            pltpu.VMEM((X, R, W), BF16),
            pltpu.VMEM((C, 8, 128), F32),
            pltpu.VMEM((XY, 8, 128), F32),
            pltpu.VMEM((Z, 8, 128), F32),
            pltpu.VMEM((H, 8, 128), F32),
            pltpu.VMEM((NDP, SP, HW), F32),
            pltpu.VMEM((NDP, SP, HW), F32),
            pltpu.VMEM((NDP, SP, HW), F32),
            pltpu.VMEM((SEQ, HW), F32),
            pltpu.VMEM((X, R, W), F32),
            pltpu.VMEM((X, R, W), F32),
            pltpu.VMEM((H, R, W), F32),
            pltpu.VMEM((NDP, 2, 128), F32),
            pltpu.VMEM((C, XY, Z, R, W), BF16),
            pltpu.VMEM((XY, 2, 128), F32),
            pltpu.VMEM((Z * C, 2, 128), F32),
            pltpu.VMEM((H, 2, 128), F32),
            pltpu.SemaphoreType.DMA((5,)),
            pltpu.SemaphoreType.DMA((NSEM,)),
            pltpu.SemaphoreType.DMA((NSEM,)),
        ],
        compiler_params=pltpu.CompilerParams(collective_id=0, has_side_effects=True),
    )(
        token_ids.reshape(1, -1), cache_lengths, embedding, ln_gain.reshape(1, -1), query_weight,
        key_cache, value_cache, out_weight, final_gain.reshape(1, -1),
    )


def solution(mesh, sizes=(4, 4, 2, 4, 4)):
    finer = Mesh(mesh.devices.reshape(sizes), DP_MP)
    placed = (
        P(),
        P(DP),
        P(DP_MP, None),
        P(),
        P(DP, MP),
        P(DP, None, MP),
        P(DP, None, MP),
        P(MP, DP),
        P(),
    )
    return jax.shard_map(
        functools.partial(per_device, sizes), mesh=finer, in_specs=placed,
        out_specs=P(None, DP_MP), check_vma=False,
    )
```

```python
import functools

import jax
import jax.numpy as jnp
from jax import lax
from jax.experimental import pallas as pl
from jax.experimental.pallas import tpu as pltpu
from jax.sharding import Mesh
from jax.sharding import PartitionSpec as P

HD = 128
EPS = 1e-5
DP_MP = ("dp_0", "dp_1", "dp_2", "mp_0", "mp_1")
DP = ("dp_0", "dp_1", "dp_2")
MP = ("mp_0", "mp_1")
MESH = pl.DeviceIdType.MESH
F32 = jnp.float32
BF16 = jnp.bfloat16
NSEM = 36


def kernel(
    sizes,
    ids_ref, len_ref, emb_ref, lng_ref, wq_ref, key_ref, val_ref, wo_ref, fg_ref,
    out_ref,
    emb, wq, key, val, wo,
    p, r1, a1, a2, a3, b1, b2, b3, t0, r3, r4, r5, s1, s2, s3, s4,
    part, rq, ra, att_all, op, ro1, ro2, gmat, dm, fb, fs, g1, g2,
    load_sem, send_sem, recv_sem,
):
    Y, Z, C, X, H = sizes
    NDP, XY, ZC, ZH = Y * Z * C, X * Y, Z * C, Z // 2
    V, D = emb.shape
    SP, T, HW = key.shape
    W = D // NDP
    SEQ = SP * NDP
    R = SEQ // X
    NH = HW // HD

    yi, zi, ci, xi, hi = (lax.axis_index(a) for a in DP_MP)
    xy = xi * Y + yi
    zz_own = hi * Z + zi
    xyc = xy * C + ci
    dp = (yi * Z + zi) * C + ci

    def xy_dev(i):
        return {"mp_0": lax.div(i, Y), "dp_0": lax.rem(i, Y)}

    def xyc_dev(i):
        return {"dp_2": lax.rem(i, C), **xy_dev(lax.div(i, C))}

    def zz_dev(i):
        return {"mp_1": lax.div(i, Z), "dp_1": lax.rem(i, Z)}

    def dp_dev(i):
        return {"dp_0": lax.div(i, ZC), "dp_1": lax.rem(lax.div(i, C), Z), "dp_2": lax.rem(i, C)}

    def y_dev(i):
        return {"dp_0": i}

    def z_dev(i):
        return {"dp_1": i}

    def c_dev(i):
        return {"dp_2": i}

    def x_dev(i):
        return {"mp_0": i}

    def h_dev(i):
        return {"mp_1": i}

    def each(n, body):
        if n <= 4:
            for k in range(1, n):
                body(k)
        else:
            lax.fori_loop(1, n, lambda k, _: body(k), None)

    def send(s, src, dst, dev):
        pltpu.make_async_remote_copy(
            src_ref=src, dst_ref=dst, send_sem=send_sem.at[s], recv_sem=recv_sem.at[s],
            device_id=dev, device_id_type=MESH,
        ).start()

    def take(sem, ref):
        pltpu.make_async_copy(ref, ref, sem).wait()

    pending = []
    used = [0]

    def new():
        used[0] += 1
        return used[0] - 1

    def arrived(s, ref):
        take(recv_sem.at[s], ref)
        pending.append((s, ref))

    def exchange(src, dst, own, n, dev):
        s = new()

        def body(k):
            i = lax.rem(own + k, n)
            send(s, src(i), dst, dev(i))

        each(n, body)
        return s

    def gather(buf, own, n, dev):
        return exchange(lambda i: buf.at[own], buf.at[own], own, n, dev)

    def to_rows(cols, start=None):
        n = cols[0].shape[0]
        lane = lax.broadcasted_iota(jnp.int32, (n, 128), 1)
        x = jnp.zeros((n, 128), F32)
        for k, col in enumerate(cols):
            x = jnp.where(lane == k, col, x)
        if start is not None:
            x = jnp.concatenate([x] * (SEQ // n), axis=0)
            r = lax.broadcasted_iota(jnp.int32, (SEQ, 128), 0)
            x = jnp.where((r >= start) & (r < start + n), x, 0.0)
        if x.shape[0] < 128:
            x = jnp.concatenate([x, jnp.zeros((128 - x.shape[0], 128), F32)], axis=0)
        return jnp.transpose(x)

    def to_cols(rows):
        row = lax.broadcasted_iota(jnp.int32, (128, 128), 0)
        x = jnp.zeros((128, 128), F32)
        for k, r in enumerate(rows):
            x = jnp.where(row == k, r, x)
        return jnp.transpose(x)

    loads = [
        pltpu.make_async_copy(a, b, load_sem.at[i])
        for i, (a, b) in enumerate(
            ((emb_ref, emb), (wq_ref, wq), (key_ref, key), (val_ref, val), (wo_ref, wo))
        )
    ]
    for c in loads:
        c.start()

    barrier = pltpu.get_barrier_semaphore()

    def greet(dev):
        pl.semaphore_signal(barrier, inc=1, device_id=dev, device_id_type=MESH)

    for kh in range(1, H):
        for kz in range(Z):
            greet({"mp_1": lax.rem(hi + kh, H), "dp_1": lax.rem(zi + kz, Z)})
    each(NDP, lambda k: greet(dp_dev(lax.rem(dp + k, NDP))))
    for kx in range(1, X):
        for ky in range(Y):
            for kc in range(C):
                greet({
                    "mp_0": lax.rem(xi + kx, X),
                    "dp_0": lax.rem(yi + ky, Y),
                    "dp_2": lax.rem(ci + kc, C),
                })
    greeted = NDP - 1 + (X - 1) * Y * C + (H - 1) * Z

    flat = (dp * X + xi) * H + hi
    ids = ids_ref[...]
    if SEQ < 128:
        ids = jnp.concatenate([ids, jnp.full((1, 128 - SEQ), -1, jnp.int32)], axis=1)
    row = lax.broadcasted_iota(jnp.int32, (128, 128), 0)
    hot = jnp.where((row + flat * V == ids) & (row < V), 1.0, 0.0).astype(F32)
    hot = jnp.transpose(hot)[:SEQ, :V].astype(BF16)

    loads[0].wait()
    other = 1 - ci
    acc = jnp.zeros((SEQ, 128), F32)

    def rows_of(acc, core, half):
        for yy in range(Y):
            for zz in range(ZH):
                b = (yy * Z + half * ZH + zz) * C + core
                cols = pl.ds(pl.multiple_of(b * W, 128), W)
                blk = jnp.dot(hot, emb[:, cols], preferred_element_type=F32)
                for j in range(0, W, 128):
                    acc = acc + blk[:, j : j + 128]
                blk = blk.astype(BF16)
                for xx in range(X):
                    p[core, half, yy, xx, zz] = blk[xx * R : (xx + 1) * R]
        return acc

    def to_core(half):
        s = new()
        send(s, p.at[other, half], r1.at[half], c_dev(other))
        return s

    def summed(half):
        for yy in range(Y):
            for xx in range(X):
                r1[half, yy, xx] = r1[half, yy, xx] + p[ci, half, yy, xx]

    acc = rows_of(acc, other, 0)
    pl.semaphore_wait(barrier, greeted)
    e1a = to_core(0)
    acc = rows_of(acc, other, 1)
    e1b = to_core(1)
    acc = rows_of(acc, ci, 0)
    arrived(e1a, r1.at[0])
    summed(0)
    ea = exchange(lambda i: r1.at[0, :, i], a1.at[xi], xi, X, x_dev)
    acc = rows_of(acc, ci, 1)
    arrived(e1b, r1.at[1])
    summed(1)
    eb = exchange(lambda i: r1.at[1, i], b1.at[yi], yi, Y, y_dev)
    a1[xi] = r1[0, :, xi]
    b1[yi] = r1[1, yi]

    mean = jnp.sum(acc, axis=1, keepdims=True) / D
    devs = []
    for xx in range(X):
        m = mean[xx * R : (xx + 1) * R]
        sq = jnp.zeros((R, 128), F32)
        for cc in range(C):
            for hh in range(2):
                for yy in range(Y):
                    for zz in range(ZH):
                        d = p[cc, hh, yy, xx, zz].astype(F32) - m
                        for j in range(0, W, 128):
                            sq = sq + d[:, j : j + 128] * d[:, j : j + 128]
        devs.append(jnp.sum(sq, axis=1, keepdims=True) / D)
    var = jnp.concatenate(devs, axis=0)
    s1[ci] = to_rows((mean, var))[:8]
    es = gather(s1, ci, C, c_dev)

    arrived(ea, a1.at[pl.ds(0, X - 1)])
    for yy in range(Y):
        tot = a1[0, yy]
        for k in range(1, X):
            tot = tot + a1[k, yy]
        a2[yy] = tot
    ea = exchange(lambda i: a2.at[i], a3.at[yi], yi, Y, y_dev)
    a3[yi] = a2[yi]
    arrived(es, s1.at[pl.ds(0, C - 1)])
    s2[xy] = jnp.sum(s1[...], axis=0)
    es = gather(s2, xy, XY, xy_dev)
    arrived(eb, b1.at[pl.ds(0, Y - 1)])
    for xx in range(X):
        tot = b1[0, xx]
        for k in range(1, Y):
            tot = tot + b1[k, xx]
        b2[xx] = tot
    eb = exchange(lambda i: b2.at[i], b3.at[xi], xi, X, x_dev)
    b3[xi] = b2[xi]

    half_row = lax.broadcasted_iota(jnp.int32, (16, W), 0)
    for j in range(NDP):
        gain = fg_ref[:, j * W : (j + 1) * W]
        high = gain.astype(BF16).astype(F32)
        both = jnp.where(half_row == 0, high, jnp.where(half_row == 1, gain - high, 0.0))
        got = lax.dot_general(
            both.astype(BF16), emb[:, j * W : (j + 1) * W], (((1,), (1,)), ((), ())),
            preferred_element_type=F32,
        )
        gmat[j : j + 1] = got[0:1] + got[1:2]

    arrived(ea, a3.at[pl.ds(0, Y - 1)])
    tot = a3[0]
    for k in range(1, Y):
        tot = tot + a3[k]
    t0[0:ZH] = tot
    arrived(eb, b3.at[pl.ds(0, X - 1)])
    tot = b3[0]
    for k in range(1, X):
        tot = tot + b3[k]
    t0[ZH:Z] = tot
    ez = exchange(lambda i: t0.at[i], r3.at[zi], zi, Z, z_dev)
    r3[zi] = t0[zi]
    arrived(es, s2.at[pl.ds(0, XY - 1)])
    s3[zi] = jnp.sum(s2[...], axis=0)
    es = gather(s3, zi, Z, z_dev)

    arrived(ez, r3.at[pl.ds(0, Z - 1)])
    tot = r3[0]
    for k in range(1, Z):
        tot = tot + r3[k]
    r4[hi] = tot
    if H > 1:
        ez = gather(r4, hi, H, h_dev)
    arrived(es, s3.at[pl.ds(0, Z - 1)])
    s4[hi] = jnp.sum(s3[...], axis=0)
    if H > 1:
        es = gather(s4, hi, H, h_dev)
        arrived(ez, r4.at[pl.ds(0, H - 1)])
    tot = r4[0]
    for k in range(1, H):
        tot = tot + r4[k]
    r5[xi] = tot
    ex = gather(r5, xi, X, x_dev)
    if H > 1:
        arrived(es, s4.at[pl.ds(0, H - 1)])
    stats = jnp.sum(s4[...], axis=0)
    stats = to_cols((stats[0:1], stats[1:2]))
    mean, var = stats[:SEQ, 0:1], stats[:SEQ, 1:2]
    arrived(ex, r5.at[pl.ds(0, X - 1)])

    own_cols = pl.ds(pl.multiple_of(dp * W, 128), W)
    embedded = r5[...].reshape(SEQ, W).astype(F32)
    normed = (lng_ref[:, own_cols] * (embedded - mean) * lax.rsqrt(var + EPS)).astype(BF16)
    loads[1].wait()
    partial = jnp.dot(normed, wq[...], preferred_element_type=F32)
    for j in range(NDP):
        part[j] = partial[j * SP : (j + 1) * SP]
    eq = exchange(lambda i: part.at[i], rq.at[dp], dp, NDP, dp_dev)
    rq[dp] = part[dp]
    loads[2].wait()
    loads[3].wait()
    arrived(eq, rq.at[pl.ds(0, NDP - 1)])
    queries = (jnp.sum(rq[...], axis=0) * HD**-0.5).astype(BF16).astype(F32)

    head = lax.broadcasted_iota(jnp.int32, (8, HW), 0) * HD
    lane = lax.broadcasted_iota(jnp.int32, (8, HW), 1)
    own_head = (lane >= head) & (lane < head + HD)
    place = lax.broadcasted_iota(jnp.int32, (8, T), 1)
    pair = lax.broadcasted_iota(jnp.int32, (SP, HW), 0)
    attended = jnp.zeros((SP, HW), F32)
    for s in range(SP):
        q = jnp.where(own_head, queries[s : s + 1], 0.0).astype(BF16)
        scores = lax.dot_general(
            q, key[s], (((1,), (1,)), ((), ())), preferred_element_type=F32
        )
        scores = jnp.where(place < len_ref[s], scores, -1e30)
        e = jnp.exp(scores - jnp.max(scores, axis=1, keepdims=True))
        w = (e / jnp.sum(e, axis=1, keepdims=True)).astype(BF16)
        got = jnp.dot(w, val[s], preferred_element_type=F32)
        got = jnp.sum(jnp.where(own_head, got, 0.0), axis=0, keepdims=True)
        attended = jnp.where(pair == s, got, attended)
    ra[dp] = attended.astype(BF16).astype(F32)
    eg = gather(ra, dp, NDP, dp_dev)
    loads[4].wait()
    arrived(eg, ra.at[pl.ds(0, NDP - 1)])
    for j in range(NDP):
        att_all[j * SP : (j + 1) * SP] = ra[j]

    mixed = jnp.dot(att_all[...].astype(BF16), wo[...], preferred_element_type=F32)
    for xx in range(X):
        op[xx] = mixed[xx * R : (xx + 1) * R]
    eo = exchange(lambda i: op.at[i], ro1.at[xi], xi, X, x_dev)
    ro1[xi] = op[xi]
    arrived(eo, ro1.at[pl.ds(0, X - 1)])
    ro2[hi] = jnp.sum(ro1[...], axis=0).astype(BF16)
    if H > 1:
        eo = gather(ro2, hi, H, h_dev)
        arrived(eo, ro2.at[pl.ds(0, H - 1)])
    hidden = r5[xi].astype(F32) + jnp.sum(ro2[...].astype(F32), axis=0)

    m = jnp.sum(hidden, axis=1, keepdims=True) / W
    d = hidden - m
    zh, zl = lax.div(zi, ZH), lax.rem(zi, ZH)
    fb[zh, ci, xi, yi, zl] = (fg_ref[:, own_cols] * d).astype(BF16)
    ef = exchange(
        lambda i: fb.at[zh, ci, xi, yi, zl], fb.at[zh, ci, xi, yi, zl], zi, Z, z_dev
    )
    fs[ci, xy, zi] = to_rows((m, jnp.sum(d * d, axis=1, keepdims=True)), xi * R)[:2]
    es = exchange(lambda i: fs.at[ci, xy, zi], fs.at[ci, xy, zi], zi, Z, z_dev)

    arrived(ef, fb.at[0, 0, 0, pl.ds(0, Z - 1), 0])
    ea = exchange(lambda i: fb.at[0, ci, xi, yi], fb.at[0, ci, xi, yi], yi, Y, y_dev)
    eb = exchange(lambda i: fb.at[1, ci, xi, yi], fb.at[1, ci, xi, yi], xi, X, x_dev)
    arrived(es, fs.at[ci, xy, pl.ds(0, Z - 1)])
    es = exchange(lambda i: fs.at[ci, xy], fs.at[ci, xy], xy, XY, xy_dev)
    arrived(ea, fb.at[0, ci, xi, pl.ds(0, Y - 1)])
    ea = exchange(lambda i: fb.at[0, ci, xi], fb.at[0, ci, xi], xi, X, x_dev)
    arrived(eb, fb.at[1, ci, pl.ds(0, X - 1), yi])
    eb = exchange(lambda i: fb.at[1, ci, :, yi], fb.at[1, ci, :, yi], yi, Y, y_dev)
    arrived(es, fs.at[ci, pl.ds(0, XY - 1)])
    es = exchange(lambda i: fs.at[ci], fs.at[ci], ci, C, c_dev)

    def products(logits, core, half):
        for yy in range(Y):
            lhs = jnp.concatenate(
                [
                    jnp.concatenate([fb[half, core, xx, yy, zz] for xx in range(X)], axis=0)
                    for zz in range(ZH)
                ],
                axis=1,
            )
            rhs = jnp.concatenate(
                [
                    emb[:, pl.ds(pl.multiple_of(
                        ((yy * Z + half * ZH + zz) * C + core) * W, 128), W)]
                    for zz in range(ZH)
                ],
                axis=1,
            )
            logits = logits + lax.dot_general(
                lhs, rhs, (((1,), (1,)), ((), ())), preferred_element_type=F32
            )
        return logits

    logits = jnp.zeros((SEQ, V), F32)
    arrived(ea, fb.at[0, ci, pl.ds(0, X - 1)])
    ea = exchange(lambda i: fb.at[0, ci], fb.at[0, ci], ci, C, c_dev)
    arrived(eb, fb.at[1, ci, :, pl.ds(0, Y - 1)])
    eb = exchange(lambda i: fb.at[1, ci], fb.at[1, ci], ci, C, c_dev)
    arrived(es, fs.at[ci])
    row_mean = jnp.zeros((1, 128), F32)
    row_var = jnp.zeros((1, 128), F32)
    blocks = []
    for yy in range(Y):
        for zz in range(Z):
            for cc in range(C):
                b = fs[cc, yy, zz]
                for xx in range(1, X):
                    b = b + fs[cc, xx * Y + yy, zz]
                row_mean = row_mean + b[0:1]
                row_var = row_var + b[1:2]
                blocks.append(b[0:1])
    row_mean = row_mean / NDP
    for j in range(NDP):
        off = blocks[j] - row_mean
        row_var = row_var + W * (off * off)
        dm[j : j + 1] = off
    scale = to_cols((lax.rsqrt(row_var / D + EPS),))[:SEQ, 0:1]
    offs = jnp.transpose(dm[...])[:SEQ, :NDP]
    logits = logits + jnp.dot(
        offs, gmat[...], preferred_element_type=F32, precision=lax.Precision.HIGHEST
    )
    logits = products(logits, ci, 0)
    logits = products(logits, ci, 1)
    arrived(ea, fb.at[0, other])
    logits = products(logits, other, 0)
    arrived(eb, fb.at[1, other])
    logits = products(logits, other, 1) * scale

    top = jnp.max(logits, axis=1, keepdims=True)
    total = jnp.sum(jnp.exp(logits - top), axis=1, keepdims=True)

    def merged(buf):
        v = buf[...]
        tops, sums = v[:, 0:1], v[:, 1:2]
        best = jnp.max(tops, axis=0)
        return best, jnp.sum(sums * jnp.exp(tops - best[None]), axis=0)

    def joined(best, tot):
        r = lax.broadcasted_iota(jnp.int32, (2, 128), 0)
        return jnp.where(r == 0, best, tot)

    g1[xyc] = to_rows((top, total))[:2]
    eg = gather(g1, xyc, XY * C, xyc_dev)
    arrived(eg, g1.at[pl.ds(0, XY * C - 1)])
    g2[zz_own] = joined(*merged(g1))
    eg = gather(g2, zz_own, Z * H, zz_dev)
    arrived(eg, g2.at[pl.ds(0, Z * H - 1)])
    best, tot = merged(g2)
    stats = to_cols((best, jnp.log(tot)))
    out_ref[...] = (logits - stats[:SEQ, 0:1]) - stats[:SEQ, 1:2]
    for s, ref in pending:
        take(send_sem.at[s], ref)


def per_device(sizes, token_ids, cache_lengths, embedding, ln_gain, query_weight, key_cache,
               value_cache, out_weight, final_gain):
    Y, Z, C, X, H = sizes
    NDP, XY, ZH = Y * Z * C, X * Y, Z // 2
    V, D = embedding.shape
    SP, T, HW = key_cache.shape
    W = D // NDP
    SEQ = SP * NDP
    R = SEQ // X
    vmem = pl.BlockSpec(memory_space=pltpu.VMEM)
    smem = pl.BlockSpec(memory_space=pltpu.SMEM)
    hbm = pl.BlockSpec(memory_space=pl.ANY)
    return pl.pallas_call(
        functools.partial(kernel, sizes),
        name="decode",
        out_shape=jax.ShapeDtypeStruct((SEQ, V), F32),
        in_specs=[vmem, smem, hbm, vmem, hbm, hbm, hbm, hbm, vmem],
        out_specs=vmem,
        scratch_shapes=[
            pltpu.VMEM((V, D), BF16),
            pltpu.VMEM((W, HW), BF16),
            pltpu.VMEM((SP, T, HW), BF16),
            pltpu.VMEM((SP, T, HW), BF16),
            pltpu.VMEM((HW, W), BF16),
            pltpu.VMEM((C, 2, Y, X, ZH, R, W), BF16),
            pltpu.VMEM((2, Y, X, ZH, R, W), BF16),
            pltpu.VMEM((X, Y, ZH, R, W), BF16),
            pltpu.VMEM((Y, ZH, R, W), BF16),
            pltpu.VMEM((Y, ZH, R, W), BF16),
            pltpu.VMEM((Y, X, ZH, R, W), BF16),
            pltpu.VMEM((X, ZH, R, W), BF16),
            pltpu.VMEM((X, ZH, R, W), BF16),
            pltpu.VMEM((Z, R, W), BF16),
            pltpu.VMEM((Z, R, W), BF16),
            pltpu.VMEM((H, R, W), BF16),
            pltpu.VMEM((X, R, W), BF16),
            pltpu.VMEM((C, 8, 128), F32),
            pltpu.VMEM((XY, 8, 128), F32),
            pltpu.VMEM((Z, 8, 128), F32),
            pltpu.VMEM((H, 8, 128), F32),
            pltpu.VMEM((NDP, SP, HW), F32),
            pltpu.VMEM((NDP, SP, HW), F32),
            pltpu.VMEM((NDP, SP, HW), F32),
            pltpu.VMEM((SEQ, HW), F32),
            pltpu.VMEM((X, R, W), F32),
            pltpu.VMEM((X, R, W), F32),
            pltpu.VMEM((H, R, W), BF16),
            pltpu.VMEM((NDP, V), F32),
            pltpu.VMEM((max(NDP, 128), 128), F32),
            pltpu.VMEM((2, C, X, Y, ZH, R, W), BF16),
            pltpu.VMEM((C, XY, Z, 2, 128), F32),
            pltpu.VMEM((XY * C, 2, 128), F32),
            pltpu.VMEM((Z * H, 2, 128), F32),
            pltpu.SemaphoreType.DMA((5,)),
            pltpu.SemaphoreType.DMA((NSEM,)),
            pltpu.SemaphoreType.DMA((NSEM,)),
        ],
        compiler_params=pltpu.CompilerParams(collective_id=0, has_side_effects=True),
    )(
        token_ids.reshape(1, -1), cache_lengths, embedding, ln_gain.reshape(1, -1), query_weight,
        key_cache, value_cache, out_weight, final_gain.reshape(1, -1),
    )


def solution(mesh, sizes=(4, 4, 2, 4, 4)):
    finer = Mesh(mesh.devices.reshape(sizes), DP_MP)
    placed = (
        P(),
        P(DP),
        P(DP_MP, None),
        P(),
        P(DP, MP),
        P(DP, None, MP),
        P(DP, None, MP),
        P(MP, DP),
        P(),
    )
    return jax.shard_map(
        functools.partial(per_device, sizes), mesh=finer, in_specs=placed,
        out_specs=P(None, DP_MP), check_vma=False,
    )
```

```python
import functools

import jax
import jax.numpy as jnp
from jax import lax
from jax.experimental import pallas as pl
from jax.experimental.pallas import tpu as pltpu
from jax.sharding import Mesh
from jax.sharding import PartitionSpec as P

HD = 128
EPS = 1e-5
DP_MP = ("dp_0", "dp_1", "dp_2", "mp_0", "mp_1")
DP = ("dp_0", "dp_1", "dp_2")
MP = ("mp_0", "mp_1")
MESH = pl.DeviceIdType.MESH
F32 = jnp.float32
BF16 = jnp.bfloat16
NSEM = 36


def kernel(
    sizes,
    ids_ref, len_ref, emb_ref, lng_ref, wq_ref, key_ref, val_ref, wo_ref, fg_ref,
    out_ref, lse_ref,
    emb, wq, key, val, wo,
    p, r1, a1, a2, a3, b1, b2, b3, t0, r3, r4, r5, s1, sx, sy, s3, s4,
    part, rq, ra, att_all, op, ro1, ro2, gmat, dm, fb, fs, g1, g2,
    load_sem, send_sem, recv_sem, ring_sem,
):
    Y, Z, C, X, H = sizes
    NDP, XY, ZC, ZH = Y * Z * C, X * Y, Z * C, Z // 2
    V, D = emb.shape
    SP, T, HW = key.shape
    W = D // NDP
    SEQ = SP * NDP
    R = SEQ // X
    NH = HW // HD

    yi, zi, ci, xi, hi = (lax.axis_index(a) for a in DP_MP)
    xy = xi * Y + yi
    zz_own = hi * Z + zi
    xyc = xy * C + ci
    dp = (yi * Z + zi) * C + ci

    def xy_dev(i):
        return {"mp_0": lax.div(i, Y), "dp_0": lax.rem(i, Y)}

    def xyc_dev(i):
        return {"dp_2": lax.rem(i, C), **xy_dev(lax.div(i, C))}

    def zz_dev(i):
        return {"mp_1": lax.div(i, Z), "dp_1": lax.rem(i, Z)}

    def dp_dev(i):
        return {"dp_0": lax.div(i, ZC), "dp_1": lax.rem(lax.div(i, C), Z), "dp_2": lax.rem(i, C)}

    def y_dev(i):
        return {"dp_0": i}

    def z_dev(i):
        return {"dp_1": i}

    def c_dev(i):
        return {"dp_2": i}

    def x_dev(i):
        return {"mp_0": i}

    def h_dev(i):
        return {"mp_1": i}

    def each(n, body):
        if n <= 4:
            for k in range(1, n):
                body(k)
        else:
            lax.fori_loop(1, n, lambda k, _: body(k), None)

    def send(s, src, dst, dev):
        pltpu.make_async_remote_copy(
            src_ref=src, dst_ref=dst, send_sem=send_sem.at[s], recv_sem=recv_sem.at[s],
            device_id=dev, device_id_type=MESH,
        ).start()

    def take(sem, ref):
        pltpu.make_async_copy(ref, ref, sem).wait()

    pending = []
    used = [0]

    def new():
        used[0] += 1
        return used[0] - 1

    def arrived(s, ref):
        take(recv_sem.at[s], ref)
        pending.append((s, ref))

    def exchange(src, dst, own, n, dev):
        s = new()

        def body(k):
            i = lax.rem(own + k, n)
            send(s, src(i), dst, dev(i))

        each(n, body)
        return s

    def gather(buf, own, n, dev):
        return exchange(lambda i: buf.at[own], buf.at[own], own, n, dev)

    def to_rows(cols, start=None):
        n = cols[0].shape[0]
        lane = lax.broadcasted_iota(jnp.int32, (n, 128), 1)
        x = jnp.zeros((n, 128), F32)
        for k, col in enumerate(cols):
            x = jnp.where(lane == k, col, x)
        if start is not None:
            x = jnp.concatenate([x] * (SEQ // n), axis=0)
            r = lax.broadcasted_iota(jnp.int32, (SEQ, 128), 0)
            x = jnp.where((r >= start) & (r < start + n), x, 0.0)
        if x.shape[0] < 128:
            x = jnp.concatenate([x, jnp.zeros((128 - x.shape[0], 128), F32)], axis=0)
        return jnp.transpose(x)

    def to_cols(rows):
        row = lax.broadcasted_iota(jnp.int32, (128, 128), 0)
        x = jnp.zeros((128, 128), F32)
        for k, r in enumerate(rows):
            x = jnp.where(row == k, r, x)
        return jnp.transpose(x)

    loads = [
        pltpu.make_async_copy(a, b, load_sem.at[i])
        for i, (a, b) in enumerate(
            ((emb_ref, emb), (wq_ref, wq), (key_ref, key), (val_ref, val), (wo_ref, wo))
        )
    ]
    for c in loads:
        c.start()

    barrier = pltpu.get_barrier_semaphore()

    def greet(dev):
        pl.semaphore_signal(barrier, inc=1, device_id=dev, device_id_type=MESH)

    ring = Z * H
    greet(c_dev(1 - ci))
    for own, n, dev in ((xi, X, x_dev), (yi, Y, y_dev), (zi, Z, z_dev)):
        for k in range(1, n):
            greet(dev(lax.rem(own + k, n)))
    for k in (1, ring - 1):
        greet(zz_dev(lax.rem(zz_own + k, ring)))
    greeted = X + Y + Z
    rounds = [d for d in (1, 2, 4, 8, 16) if 2 * d < ring]

    def tell(r):
        if r < len(rounds):
            for k in (rounds[r], ring - rounds[r]):
                pl.semaphore_signal(
                    ring_sem.at[r], inc=1, device_id=zz_dev(lax.rem(zz_own + k, ring)),
                    device_id_type=MESH,
                )

    def told(r):
        if r < len(rounds):
            pl.semaphore_wait(ring_sem.at[r], 2)

    flat = (dp * X + xi) * H + hi
    ids = ids_ref[...]
    if SEQ < 128:
        ids = jnp.concatenate([ids, jnp.full((1, 128 - SEQ), -1, jnp.int32)], axis=1)
    row = lax.broadcasted_iota(jnp.int32, (128, 128), 0)
    hot = jnp.where((row + flat * V == ids) & (row < V), 1.0, 0.0).astype(F32)
    hot = jnp.transpose(hot)[:SEQ, :V].astype(BF16)

    loads[0].wait()
    other = 1 - ci
    acc = jnp.zeros((SEQ, 128), F32)

    def rows_of(acc, core, half):
        for yy in range(Y):
            for zz in range(ZH):
                b = (yy * Z + half * ZH + zz) * C + core
                cols = pl.ds(pl.multiple_of(b * W, 128), W)
                blk = jnp.dot(hot, emb[:, cols], preferred_element_type=F32)
                for j in range(0, W, 128):
                    acc = acc + blk[:, j : j + 128]
                blk = blk.astype(BF16)
                for xx in range(X):
                    p[core, half, yy, xx, zz] = blk[xx * R : (xx + 1) * R]
        return acc

    def to_core(half):
        s = new()
        send(s, p.at[other, half], r1.at[half], c_dev(other))
        return s

    def summed(half):
        for yy in range(Y):
            for xx in range(X):
                r1[half, yy, xx] = r1[half, yy, xx] + p[ci, half, yy, xx]

    acc = rows_of(acc, other, 0)
    pl.semaphore_wait(barrier, greeted)
    e1a = to_core(0)
    tell(0)
    acc = rows_of(acc, other, 1)
    e1b = to_core(1)
    acc = rows_of(acc, ci, 0)
    told(0)
    tell(1)
    arrived(e1a, r1.at[0])
    summed(0)
    ea = exchange(lambda i: r1.at[0, :, i], a1.at[xi], xi, X, x_dev)
    acc = rows_of(acc, ci, 1)
    arrived(e1b, r1.at[1])
    summed(1)
    eb = exchange(lambda i: r1.at[1, i], b1.at[yi], yi, Y, y_dev)
    a1[xi] = r1[0, :, xi]
    b1[yi] = r1[1, yi]

    mean = jnp.sum(acc, axis=1, keepdims=True) / D
    devs = []
    for xx in range(X):
        m = mean[xx * R : (xx + 1) * R]
        sq = jnp.zeros((R, 128), F32)
        for cc in range(C):
            for hh in range(2):
                for yy in range(Y):
                    for zz in range(ZH):
                        d = p[cc, hh, yy, xx, zz].astype(F32) - m
                        for j in range(0, W, 128):
                            sq = sq + d[:, j : j + 128] * d[:, j : j + 128]
        devs.append(jnp.sum(sq, axis=1, keepdims=True) / D)
    var = jnp.concatenate(devs, axis=0)
    s1[ci] = to_rows((mean, var))[:8]
    es = gather(s1, ci, C, c_dev)
    told(1)
    tell(2)

    arrived(ea, a1.at[pl.ds(0, X - 1)])
    for yy in range(Y):
        tot = a1[0, yy]
        for k in range(1, X):
            tot = tot + a1[k, yy]
        a2[yy] = tot
    ea = exchange(lambda i: a2.at[i], a3.at[yi], yi, Y, y_dev)
    a3[yi] = a2[yi]
    arrived(es, s1.at[pl.ds(0, C - 1)])
    sx[xi] = jnp.sum(s1[...], axis=0)
    es = gather(sx, xi, X, x_dev)
    arrived(eb, b1.at[pl.ds(0, Y - 1)])
    for xx in range(X):
        tot = b1[0, xx]
        for k in range(1, Y):
            tot = tot + b1[k, xx]
        b2[xx] = tot
    eb = exchange(lambda i: b2.at[i], b3.at[xi], xi, X, x_dev)
    b3[xi] = b2[xi]
    arrived(es, sx.at[pl.ds(0, X - 1)])
    sy[yi] = jnp.sum(sx[...], axis=0)
    es = gather(sy, yi, Y, y_dev)

    half_row = lax.broadcasted_iota(jnp.int32, (16, W), 0)
    for j in range(NDP):
        gain = fg_ref[:, j * W : (j + 1) * W]
        high = gain.astype(BF16).astype(F32)
        both = jnp.where(half_row == 0, high, jnp.where(half_row == 1, gain - high, 0.0))
        got = lax.dot_general(
            both.astype(BF16), emb[:, j * W : (j + 1) * W], (((1,), (1,)), ((), ())),
            preferred_element_type=F32,
        )
        gmat[j : j + 1] = got[0:1] + got[1:2]

    arrived(ea, a3.at[pl.ds(0, Y - 1)])
    tot = a3[0]
    for k in range(1, Y):
        tot = tot + a3[k]
    t0[0:ZH] = tot
    arrived(eb, b3.at[pl.ds(0, X - 1)])
    tot = b3[0]
    for k in range(1, X):
        tot = tot + b3[k]
    t0[ZH:Z] = tot
    ez = exchange(lambda i: t0.at[i], r3.at[zi], zi, Z, z_dev)
    r3[zi] = t0[zi]
    arrived(es, sy.at[pl.ds(0, Y - 1)])
    s3[zi] = jnp.sum(sy[...], axis=0)
    es = gather(s3, zi, Z, z_dev)

    arrived(ez, r3.at[pl.ds(0, Z - 1)])
    tot = r3[0]
    for k in range(1, Z):
        tot = tot + r3[k]
    r4[hi] = tot
    told(2)
    if H > 1:
        ez = gather(r4, hi, H, h_dev)
    arrived(es, s3.at[pl.ds(0, Z - 1)])
    s4[hi] = jnp.sum(s3[...], axis=0)
    if H > 1:
        es = gather(s4, hi, H, h_dev)
        arrived(ez, r4.at[pl.ds(0, H - 1)])
    tot = r4[0]
    for k in range(1, H):
        tot = tot + r4[k]
    r5[xi] = tot
    ex = gather(r5, xi, X, x_dev)
    if H > 1:
        arrived(es, s4.at[pl.ds(0, H - 1)])
    stats = jnp.sum(s4[...], axis=0)
    stats = to_cols((stats[0:1], stats[1:2]))
    mean, var = stats[:SEQ, 0:1], stats[:SEQ, 1:2]
    arrived(ex, r5.at[pl.ds(0, X - 1)])

    own_cols = pl.ds(pl.multiple_of(dp * W, 128), W)
    embedded = r5[...].reshape(SEQ, W).astype(F32)
    normed = (lng_ref[:, own_cols] * (embedded - mean) * lax.rsqrt(var + EPS)).astype(BF16)
    loads[1].wait()
    partial = jnp.dot(normed, wq[...], preferred_element_type=F32)
    for j in range(NDP):
        part[j] = partial[j * SP : (j + 1) * SP]
    eq = exchange(lambda i: part.at[i], rq.at[dp], dp, NDP, dp_dev)
    rq[dp] = part[dp]
    loads[2].wait()
    loads[3].wait()
    arrived(eq, rq.at[pl.ds(0, NDP - 1)])
    queries = (jnp.sum(rq[...], axis=0) * HD**-0.5).astype(BF16).astype(F32)

    head = lax.broadcasted_iota(jnp.int32, (8, HW), 0) * HD
    lane = lax.broadcasted_iota(jnp.int32, (8, HW), 1)
    own_head = (lane >= head) & (lane < head + HD)
    place = lax.broadcasted_iota(jnp.int32, (8, T), 1)
    pair = lax.broadcasted_iota(jnp.int32, (SP, HW), 0)
    attended = jnp.zeros((SP, HW), F32)
    for s in range(SP):
        q = jnp.where(own_head, queries[s : s + 1], 0.0).astype(BF16)
        scores = lax.dot_general(
            q, key[s], (((1,), (1,)), ((), ())), preferred_element_type=F32
        )
        scores = jnp.where(place < len_ref[s], scores, -1e30)
        e = jnp.exp(scores - jnp.max(scores, axis=1, keepdims=True))
        w = (e / jnp.sum(e, axis=1, keepdims=True)).astype(BF16)
        got = jnp.dot(w, val[s], preferred_element_type=F32)
        got = jnp.sum(jnp.where(own_head, got, 0.0), axis=0, keepdims=True)
        attended = jnp.where(pair == s, got, attended)
    ra[dp] = attended.astype(BF16).astype(F32)
    eg = gather(ra, dp, NDP, dp_dev)
    loads[4].wait()
    arrived(eg, ra.at[pl.ds(0, NDP - 1)])
    for j in range(NDP):
        att_all[j * SP : (j + 1) * SP] = ra[j]

    mixed = jnp.dot(att_all[...].astype(BF16), wo[...], preferred_element_type=F32)
    for xx in range(X):
        op[xx] = mixed[xx * R : (xx + 1) * R]
    eo = exchange(lambda i: op.at[i], ro1.at[xi], xi, X, x_dev)
    ro1[xi] = op[xi]
    arrived(eo, ro1.at[pl.ds(0, X - 1)])
    ro2[hi] = jnp.sum(ro1[...], axis=0).astype(BF16)
    if H > 1:
        eo = gather(ro2, hi, H, h_dev)
        arrived(eo, ro2.at[pl.ds(0, H - 1)])
    hidden = r5[xi].astype(F32) + jnp.sum(ro2[...].astype(F32), axis=0)

    m = jnp.sum(hidden, axis=1, keepdims=True) / W
    d = hidden - m
    zh, zl = lax.div(zi, ZH), lax.rem(zi, ZH)
    fb[zh, ci, xi, yi, zl] = (fg_ref[:, own_cols] * d).astype(BF16)
    ef = exchange(
        lambda i: fb.at[zh, ci, xi, yi, zl], fb.at[zh, ci, xi, yi, zl], zi, Z, z_dev
    )
    fs[ci, xy, zi] = to_rows((m, jnp.sum(d * d, axis=1, keepdims=True)), xi * R)[:2]
    es = exchange(lambda i: fs.at[ci, xy, zi], fs.at[ci, xy, zi], zi, Z, z_dev)

    arrived(ef, fb.at[0, 0, 0, pl.ds(0, Z - 1), 0])
    ea = exchange(lambda i: fb.at[0, ci, xi, yi], fb.at[0, ci, xi, yi], yi, Y, y_dev)
    eb = exchange(lambda i: fb.at[1, ci, xi, yi], fb.at[1, ci, xi, yi], xi, X, x_dev)
    arrived(es, fs.at[ci, xy, pl.ds(0, Z - 1)])
    es = exchange(lambda i: fs.at[ci, xy], fs.at[ci, xy], xy, XY, xy_dev)
    arrived(ea, fb.at[0, ci, xi, pl.ds(0, Y - 1)])
    ea = exchange(lambda i: fb.at[0, ci, xi], fb.at[0, ci, xi], xi, X, x_dev)
    arrived(eb, fb.at[1, ci, pl.ds(0, X - 1), yi])
    eb = exchange(lambda i: fb.at[1, ci, :, yi], fb.at[1, ci, :, yi], yi, Y, y_dev)
    arrived(es, fs.at[ci, pl.ds(0, XY - 1)])
    es = exchange(lambda i: fs.at[ci], fs.at[ci], ci, C, c_dev)
    arrived(es, fs.at[ci])
    row_mean = jnp.zeros((1, 128), F32)
    row_var = jnp.zeros((1, 128), F32)
    blocks = []
    for yy in range(Y):
        for zz in range(Z):
            for cc in range(C):
                b = fs[cc, yy, zz]
                for xx in range(1, X):
                    b = b + fs[cc, xx * Y + yy, zz]
                row_mean = row_mean + b[0:1]
                row_var = row_var + b[1:2]
                blocks.append(b[0:1])
    row_mean = row_mean / NDP
    for j in range(NDP):
        off = blocks[j] - row_mean
        row_var = row_var + W * (off * off)
        dm[j : j + 1] = off
    scale = to_cols((lax.rsqrt(row_var / D + EPS),))[:SEQ, 0:1]
    offs = jnp.transpose(dm[...])[:SEQ, :NDP]
    logits = jnp.dot(
        offs, gmat[...], preferred_element_type=F32, precision=lax.Precision.HIGHEST
    )

    def products(logits, core, half):
        for yy in range(Y):
            lhs = jnp.concatenate(
                [
                    jnp.concatenate([fb[half, core, xx, yy, zz] for xx in range(X)], axis=0)
                    for zz in range(ZH)
                ],
                axis=1,
            )
            rhs = jnp.concatenate(
                [
                    emb[:, pl.ds(pl.multiple_of(
                        ((yy * Z + half * ZH + zz) * C + core) * W, 128), W)]
                    for zz in range(ZH)
                ],
                axis=1,
            )
            logits = logits + lax.dot_general(
                lhs, rhs, (((1,), (1,)), ((), ())), preferred_element_type=F32
            )
        return logits

    arrived(ea, fb.at[0, ci, pl.ds(0, X - 1)])
    ea = exchange(lambda i: fb.at[0, ci], fb.at[0, ci], ci, C, c_dev)
    arrived(eb, fb.at[1, ci, :, pl.ds(0, Y - 1)])
    eb = exchange(lambda i: fb.at[1, ci], fb.at[1, ci], ci, C, c_dev)
    logits = products(logits, ci, 0)
    logits = products(logits, ci, 1)
    arrived(ea, fb.at[0, other])
    logits = products(logits, other, 0)
    arrived(eb, fb.at[1, other])
    logits = products(logits, other, 1) * scale

    top = jnp.max(logits, axis=1, keepdims=True)
    total = jnp.sum(jnp.exp(logits - top), axis=1, keepdims=True)

    def merged(buf):
        v = buf[...]
        tops, sums = v[:, 0:1], v[:, 1:2]
        best = jnp.max(tops, axis=0)
        return best, jnp.sum(sums * jnp.exp(tops - best[None]), axis=0)

    def joined(best, tot):
        r = lax.broadcasted_iota(jnp.int32, (2, 128), 0)
        return jnp.where(r == 0, best, tot)

    g1[xyc] = to_rows((top, total))[:2]
    eg = gather(g1, xyc, XY * C, xyc_dev)
    arrived(eg, g1.at[pl.ds(0, XY * C - 1)])
    g2[zz_own] = joined(*merged(g1))
    eg = gather(g2, zz_own, Z * H, zz_dev)
    arrived(eg, g2.at[pl.ds(0, Z * H - 1)])
    best, tot = merged(g2)
    stats = to_cols((best, jnp.log(tot)))[:SEQ]
    out_ref[...] = logits - stats[:, 0:1]
    lse_ref[...] = jnp.broadcast_to(stats[:, 1:2], (SEQ, V))
    for s, ref in pending:
        take(send_sem.at[s], ref)


def per_device(sizes, token_ids, cache_lengths, embedding, ln_gain, query_weight, key_cache,
               value_cache, out_weight, final_gain):
    Y, Z, C, X, H = sizes
    NDP, XY, ZH = Y * Z * C, X * Y, Z // 2
    V, D = embedding.shape
    SP, T, HW = key_cache.shape
    W = D // NDP
    SEQ = SP * NDP
    R = SEQ // X
    vmem = pl.BlockSpec(memory_space=pltpu.VMEM)
    smem = pl.BlockSpec(memory_space=pltpu.SMEM)
    hbm = pl.BlockSpec(memory_space=pl.ANY)
    logits, lse = pl.pallas_call(
        functools.partial(kernel, sizes),
        name="decode",
        out_shape=(
            jax.ShapeDtypeStruct((SEQ, V), F32),
            jax.ShapeDtypeStruct((SEQ, V), F32),
        ),
        in_specs=[vmem, smem, hbm, vmem, hbm, hbm, hbm, hbm, vmem],
        out_specs=(vmem, vmem),
        scratch_shapes=[
            pltpu.VMEM((V, D), BF16),
            pltpu.VMEM((W, HW), BF16),
            pltpu.VMEM((SP, T, HW), BF16),
            pltpu.VMEM((SP, T, HW), BF16),
            pltpu.VMEM((HW, W), BF16),
            pltpu.VMEM((C, 2, Y, X, ZH, R, W), BF16),
            pltpu.VMEM((2, Y, X, ZH, R, W), BF16),
            pltpu.VMEM((X, Y, ZH, R, W), BF16),
            pltpu.VMEM((Y, ZH, R, W), BF16),
            pltpu.VMEM((Y, ZH, R, W), BF16),
            pltpu.VMEM((Y, X, ZH, R, W), BF16),
            pltpu.VMEM((X, ZH, R, W), BF16),
            pltpu.VMEM((X, ZH, R, W), BF16),
            pltpu.VMEM((Z, R, W), BF16),
            pltpu.VMEM((Z, R, W), BF16),
            pltpu.VMEM((H, R, W), BF16),
            pltpu.VMEM((X, R, W), BF16),
            pltpu.VMEM((C, 8, 128), F32),
            pltpu.VMEM((X, 8, 128), F32),
            pltpu.VMEM((Y, 8, 128), F32),
            pltpu.VMEM((Z, 8, 128), F32),
            pltpu.VMEM((H, 8, 128), F32),
            pltpu.VMEM((NDP, SP, HW), F32),
            pltpu.VMEM((NDP, SP, HW), F32),
            pltpu.VMEM((NDP, SP, HW), F32),
            pltpu.VMEM((SEQ, HW), F32),
            pltpu.VMEM((X, R, W), F32),
            pltpu.VMEM((X, R, W), F32),
            pltpu.VMEM((H, R, W), BF16),
            pltpu.VMEM((NDP, V), F32),
            pltpu.VMEM((max(NDP, 128), 128), F32),
            pltpu.VMEM((2, C, X, Y, ZH, R, W), BF16),
            pltpu.VMEM((C, XY, Z, 2, 128), F32),
            pltpu.VMEM((XY * C, 2, 128), F32),
            pltpu.VMEM((Z * H, 2, 128), F32),
            pltpu.SemaphoreType.DMA((5,)),
            pltpu.SemaphoreType.DMA((NSEM,)),
            pltpu.SemaphoreType.DMA((NSEM,)),
            pltpu.SemaphoreType.REGULAR((5,)),
        ],
        compiler_params=pltpu.CompilerParams(collective_id=0, has_side_effects=True),
    )(
        token_ids.reshape(1, -1), cache_lengths, embedding, ln_gain.reshape(1, -1), query_weight,
        key_cache, value_cache, out_weight, final_gain.reshape(1, -1),
    )
    return logits - lse


def solution(mesh, sizes=(4, 4, 2, 4, 4)):
    finer = Mesh(mesh.devices.reshape(sizes), DP_MP)
    placed = (
        P(),
        P(DP),
        P(DP_MP, None),
        P(),
        P(DP, MP),
        P(DP, None, MP),
        P(DP, None, MP),
        P(MP, DP),
        P(),
    )
    return jax.shard_map(
        functools.partial(per_device, sizes), mesh=finer, in_specs=placed,
        out_specs=P(None, DP_MP), check_vma=False,
    )
```

```python
import functools

import jax
import jax.numpy as jnp
from jax import lax
from jax.experimental import pallas as pl
from jax.experimental.pallas import tpu as pltpu
from jax.sharding import Mesh
from jax.sharding import PartitionSpec as P

HD = 128
EPS = 1e-5
DP_MP = ("dp_0", "dp_1", "dp_2", "mp_0", "mp_1")
DP = ("dp_0", "dp_1", "dp_2")
MP = ("mp_0", "mp_1")
MESH = pl.DeviceIdType.MESH
F32 = jnp.float32
BF16 = jnp.bfloat16
NSEM = 56


def kernel(
    sizes,
    ids_ref, len_ref, emb_ref, lng_ref, wq_ref, key_ref, val_ref, wo_ref, fg_ref,
    out_ref, lse_ref,
    emb, wq, key, val, wo,
    p, r1, a1, a2, a3, b1, b2, b3, t0, r3, r4, r5, s1, sx, sy, s3, s4,
    part, rq, ra, att_all, op, ro1, ro2, gmat, dm, fb, fs, g1, g2,
    load_sem, send_sem, recv_sem, ring_sem,
):
    Y, Z, C, X, H = sizes
    NDP, XY, ZC, ZH = Y * Z * C, X * Y, Z * C, Z // 2
    V, D = emb.shape
    SP, T, HW = key.shape
    W = D // NDP
    SEQ = SP * NDP
    R = SEQ // X
    NH = HW // HD

    yi, zi, ci, xi, hi = (lax.axis_index(a) for a in DP_MP)
    xy = xi * Y + yi
    zz_own = hi * Z + zi
    xyc = xy * C + ci
    dp = (yi * Z + zi) * C + ci

    def xy_dev(i):
        return {"mp_0": lax.div(i, Y), "dp_0": lax.rem(i, Y)}

    def xyc_dev(i):
        return {"dp_2": lax.rem(i, C), **xy_dev(lax.div(i, C))}

    def zz_dev(i):
        return {"mp_1": lax.div(i, Z), "dp_1": lax.rem(i, Z)}

    def dp_dev(i):
        return {"dp_0": lax.div(i, ZC), "dp_1": lax.rem(lax.div(i, C), Z), "dp_2": lax.rem(i, C)}

    def y_dev(i):
        return {"dp_0": i}

    def z_dev(i):
        return {"dp_1": i}

    def c_dev(i):
        return {"dp_2": i}

    def x_dev(i):
        return {"mp_0": i}

    def h_dev(i):
        return {"mp_1": i}

    def each(n, body):
        if n <= 4:
            for k in range(1, n):
                body(k)
        else:
            lax.fori_loop(1, n, lambda k, _: body(k), None)

    def send(s, src, dst, dev):
        pltpu.make_async_remote_copy(
            src_ref=src, dst_ref=dst, send_sem=send_sem.at[s], recv_sem=recv_sem.at[s],
            device_id=dev, device_id_type=MESH,
        ).start()

    def take(sem, ref):
        pltpu.make_async_copy(ref, ref, sem).wait()

    pending = []
    used = [0]

    def new():
        used[0] += 1
        return used[0] - 1

    def arrived(s, ref):
        take(recv_sem.at[s], ref)
        pending.append((s, ref))

    def exchange(src, dst, own, n, dev):
        s = new()

        def body(k):
            i = lax.rem(own + k, n)
            send(s, src(i), dst, dev(i))

        each(n, body)
        return s

    def gather(buf, own, n, dev):
        return exchange(lambda i: buf.at[own], buf.at[own], own, n, dev)

    def to_rows(cols, start=None):
        n = cols[0].shape[0]
        lane = lax.broadcasted_iota(jnp.int32, (n, 128), 1)
        x = jnp.zeros((n, 128), F32)
        for k, col in enumerate(cols):
            x = jnp.where(lane == k, col, x)
        if start is not None:
            x = jnp.concatenate([x] * (SEQ // n), axis=0)
            r = lax.broadcasted_iota(jnp.int32, (SEQ, 128), 0)
            x = jnp.where((r >= start) & (r < start + n), x, 0.0)
        if x.shape[0] < 128:
            x = jnp.concatenate([x, jnp.zeros((128 - x.shape[0], 128), F32)], axis=0)
        return jnp.transpose(x)

    def to_cols(rows):
        row = lax.broadcasted_iota(jnp.int32, (128, 128), 0)
        x = jnp.zeros((128, 128), F32)
        for k, r in enumerate(rows):
            x = jnp.where(row == k, r, x)
        return jnp.transpose(x)

    wide = Z * C * W
    pairs = [
        (emb_ref.at[:, pl.ds(k * wide, wide)], emb.at[:, pl.ds(k * wide, wide)]) for k in range(Y)
    ]
    pairs += [(wq_ref, wq), (key_ref, key), (val_ref, val), (wo_ref, wo)]
    loads = [pltpu.make_async_copy(a, b, load_sem.at[k]) for k, (a, b) in enumerate(pairs)]
    for c in loads:
        c.start()

    barrier = pltpu.get_barrier_semaphore()

    def greet(dev):
        pl.semaphore_signal(barrier, inc=1, device_id=dev, device_id_type=MESH)

    ring = Z * H
    greet(c_dev(1 - ci))
    for own, n, dev in ((xi, X, x_dev), (yi, Y, y_dev), (zi, Z, z_dev)):
        for k in range(1, n):
            greet(dev(lax.rem(own + k, n)))
    for k in (1, ring - 1):
        greet(zz_dev(lax.rem(zz_own + k, ring)))
    greeted = X + Y + Z
    rounds = [d for d in (1, 2, 4, 8, 16) if 2 * d < ring]

    def tell(r):
        if r < len(rounds):
            for k in (rounds[r], ring - rounds[r]):
                pl.semaphore_signal(
                    ring_sem.at[r], inc=1, device_id=zz_dev(lax.rem(zz_own + k, ring)),
                    device_id_type=MESH,
                )

    def told(r):
        if r < len(rounds):
            pl.semaphore_wait(ring_sem.at[r], 2)

    flat = (dp * X + xi) * H + hi
    ids = ids_ref[...]
    if SEQ < 128:
        ids = jnp.concatenate([ids, jnp.full((1, 128 - SEQ), -1, jnp.int32)], axis=1)
    row = lax.broadcasted_iota(jnp.int32, (128, 128), 0)
    hot = jnp.where((row + flat * V == ids) & (row < V), 1.0, 0.0).astype(F32)
    hot = jnp.transpose(hot)[:SEQ, :V].astype(BF16)

    other = 1 - ci
    acc = jnp.zeros((SEQ, 128), F32)
    order = [half * ZH + k for k in range(ZH) for half in (0, 1)]

    def rows_of(acc, core, zz, first):
        for yy in range(Y):
            if first:
                loads[yy].wait()
            b = (yy * Z + zz) * C + core
            cols = pl.ds(pl.multiple_of(b * W, 128), W)
            blk = jnp.dot(hot, emb[:, cols], preferred_element_type=F32)
            for j in range(0, W, 128):
                acc = acc + blk[:, j : j + 128]
            blk = blk.astype(BF16)
            for xx in range(X):
                p[core, zz, yy, xx] = blk[xx * R : (xx + 1) * R]
        return acc

    e1, ph = {}, {}
    for n, zz in enumerate(order):
        acc = rows_of(acc, other, zz, n == 0)
        if n == 0:
            pl.semaphore_wait(barrier, greeted)
        e1[zz] = new()
        send(e1[zz], p.at[other, zz], r1.at[zz], c_dev(other))
        if n == 0:
            tell(0)
    for n, zz in enumerate(order):
        acc = rows_of(acc, ci, zz, False)
        arrived(e1[zz], r1.at[zz])
        for yy in range(Y):
            for xx in range(X):
                r1[zz, yy, xx] = r1[zz, yy, xx] + p[ci, zz, yy, xx]
        if zz < ZH:
            ph[zz] = exchange(lambda i: r1.at[zz, :, i], a1.at[zz, xi], xi, X, x_dev)
            a1[zz, xi] = r1[zz, :, xi]
        else:
            ph[zz] = exchange(lambda i: r1.at[zz, i], b1.at[zz - ZH, yi], yi, Y, y_dev)
            b1[zz - ZH, yi] = r1[zz, yi]
        if n == 0:
            told(0)
            tell(1)

    mean = jnp.sum(acc, axis=1, keepdims=True) / D
    devs = []
    for xx in range(X):
        m = mean[xx * R : (xx + 1) * R]
        sq = jnp.zeros((R, 128), F32)
        for cc in range(C):
            for zz in range(Z):
                for yy in range(Y):
                    d = p[cc, zz, yy, xx].astype(F32) - m
                    for j in range(0, W, 128):
                        sq = sq + d[:, j : j + 128] * d[:, j : j + 128]
        devs.append(jnp.sum(sq, axis=1, keepdims=True) / D)
    var = jnp.concatenate(devs, axis=0)
    s1[ci] = to_rows((mean, var))[:8]
    es = gather(s1, ci, C, c_dev)
    told(1)
    tell(2)

    for n, zz in enumerate(order):
        if zz < ZH:
            arrived(ph[zz], a1.at[zz, pl.ds(0, X - 1)])
            for yy in range(Y):
                tot = a1[zz, 0, yy]
                for k in range(1, X):
                    tot = tot + a1[zz, k, yy]
                a2[zz, yy] = tot
            ph[zz] = exchange(lambda i: a2.at[zz, i], a3.at[zz, yi], yi, Y, y_dev)
            a3[zz, yi] = a2[zz, yi]
        else:
            k0 = zz - ZH
            arrived(ph[zz], b1.at[k0, pl.ds(0, Y - 1)])
            for xx in range(X):
                tot = b1[k0, 0, xx]
                for k in range(1, Y):
                    tot = tot + b1[k0, k, xx]
                b2[k0, xx] = tot
            ph[zz] = exchange(lambda i: b2.at[k0, i], b3.at[k0, xi], xi, X, x_dev)
            b3[k0, xi] = b2[k0, xi]
        if n == 0:
            arrived(es, s1.at[pl.ds(0, C - 1)])
            sx[xi] = jnp.sum(s1[...], axis=0)
            es = gather(sx, xi, X, x_dev)
    arrived(es, sx.at[pl.ds(0, X - 1)])
    sy[yi] = jnp.sum(sx[...], axis=0)
    es = gather(sy, yi, Y, y_dev)

    half_row = lax.broadcasted_iota(jnp.int32, (16, W), 0)
    for j in range(NDP):
        gain = fg_ref[:, j * W : (j + 1) * W]
        high = gain.astype(BF16).astype(F32)
        both = jnp.where(half_row == 0, high, jnp.where(half_row == 1, gain - high, 0.0))
        got = lax.dot_general(
            both.astype(BF16), emb[:, j * W : (j + 1) * W], (((1,), (1,)), ((), ())),
            preferred_element_type=F32,
        )
        gmat[j : j + 1] = got[0:1] + got[1:2]

    ez = new()
    for zz in order:
        if zz < ZH:
            buf, cnt, k0 = a3, Y, zz
        else:
            buf, cnt, k0 = b3, X, zz - ZH
        arrived(ph[zz], buf.at[k0, pl.ds(0, cnt - 1)])
        tot = buf[k0, 0]
        for k in range(1, cnt):
            tot = tot + buf[k0, k]
        t0[zz] = tot

        @pl.when(zi != zz)
        def _():
            send(ez, t0.at[zz], r3.at[zi], z_dev(jnp.int32(zz)))

    r3[zi] = t0[zi]
    arrived(es, sy.at[pl.ds(0, Y - 1)])
    s3[zi] = jnp.sum(sy[...], axis=0)
    es = gather(s3, zi, Z, z_dev)

    arrived(ez, r3.at[pl.ds(0, Z - 1)])
    tot = r3[0]
    for k in range(1, Z):
        tot = tot + r3[k]
    r4[hi] = tot
    told(2)
    if H > 1:
        ez = gather(r4, hi, H, h_dev)
    arrived(es, s3.at[pl.ds(0, Z - 1)])
    s4[hi] = jnp.sum(s3[...], axis=0)
    if H > 1:
        es = gather(s4, hi, H, h_dev)
        arrived(ez, r4.at[pl.ds(0, H - 1)])
    tot = r4[0]
    for k in range(1, H):
        tot = tot + r4[k]
    r5[xi] = tot
    ex = gather(r5, xi, X, x_dev)
    if H > 1:
        arrived(es, s4.at[pl.ds(0, H - 1)])
    stats = jnp.sum(s4[...], axis=0)
    stats = to_cols((stats[0:1], stats[1:2]))
    mean, var = stats[:SEQ, 0:1], stats[:SEQ, 1:2]
    arrived(ex, r5.at[pl.ds(0, X - 1)])

    own_cols = pl.ds(pl.multiple_of(dp * W, 128), W)
    embedded = r5[...].reshape(SEQ, W).astype(F32)
    normed = (lng_ref[:, own_cols] * (embedded - mean) * lax.rsqrt(var + EPS)).astype(BF16)
    loads[Y].wait()
    partial = jnp.dot(normed, wq[...], preferred_element_type=F32)
    for j in range(NDP):
        part[j] = partial[j * SP : (j + 1) * SP]
    eq = exchange(lambda i: part.at[i], rq.at[dp], dp, NDP, dp_dev)
    rq[dp] = part[dp]
    loads[Y + 1].wait()
    loads[Y + 2].wait()
    arrived(eq, rq.at[pl.ds(0, NDP - 1)])
    queries = (jnp.sum(rq[...], axis=0) * HD**-0.5).astype(BF16).astype(F32)

    head = lax.broadcasted_iota(jnp.int32, (8, HW), 0) * HD
    lane = lax.broadcasted_iota(jnp.int32, (8, HW), 1)
    own_head = (lane >= head) & (lane < head + HD)
    place = lax.broadcasted_iota(jnp.int32, (8, T), 1)
    pair = lax.broadcasted_iota(jnp.int32, (SP, HW), 0)
    attended = jnp.zeros((SP, HW), F32)
    for s in range(SP):
        q = jnp.where(own_head, queries[s : s + 1], 0.0).astype(BF16)
        scores = lax.dot_general(
            q, key[s], (((1,), (1,)), ((), ())), preferred_element_type=F32
        )
        scores = jnp.where(place < len_ref[s], scores, -1e30)
        e = jnp.exp(scores - jnp.max(scores, axis=1, keepdims=True))
        w = (e / jnp.sum(e, axis=1, keepdims=True)).astype(BF16)
        got = jnp.dot(w, val[s], preferred_element_type=F32)
        got = jnp.sum(jnp.where(own_head, got, 0.0), axis=0, keepdims=True)
        attended = jnp.where(pair == s, got, attended)
    ra[dp] = attended.astype(BF16)
    eg = gather(ra, dp, NDP, dp_dev)
    loads[Y + 3].wait()
    arrived(eg, ra.at[pl.ds(0, NDP - 1)])
    for j in range(NDP):
        att_all[j * SP : (j + 1) * SP] = ra[j].astype(F32)

    mixed = jnp.dot(att_all[...].astype(BF16), wo[...], preferred_element_type=F32)
    for xx in range(X):
        op[xx] = mixed[xx * R : (xx + 1) * R]
    eo = exchange(lambda i: op.at[i], ro1.at[xi], xi, X, x_dev)
    ro1[xi] = op[xi]
    arrived(eo, ro1.at[pl.ds(0, X - 1)])
    ro2[hi] = jnp.sum(ro1[...], axis=0).astype(BF16)
    if H > 1:
        eo = gather(ro2, hi, H, h_dev)
        arrived(eo, ro2.at[pl.ds(0, H - 1)])
    hidden = r5[xi].astype(F32) + jnp.sum(ro2[...].astype(F32), axis=0)

    m = jnp.sum(hidden, axis=1, keepdims=True) / W
    d = hidden - m
    fb[zi, ci, xi, yi] = (fg_ref[:, own_cols] * d).astype(BF16)
    ef = exchange(lambda i: fb.at[zi, ci, xi, yi], fb.at[zi, ci, xi, yi], zi, Z, z_dev)
    fs[ci, xy, zi] = to_rows((m, jnp.sum(d * d, axis=1, keepdims=True)), xi * R)[:2]
    es = exchange(lambda i: fs.at[ci, xy, zi], fs.at[ci, xy, zi], zi, Z, z_dev)

    arrived(ef, fb.at[pl.ds(0, Z - 1), 0, 0, 0])
    for zz in order:
        own = fb.at[zz, ci, xi, yi]
        own_n_dev = (yi, Y, y_dev) if zz < ZH else (xi, X, x_dev)
        ph[zz] = exchange(lambda i: own, own, *own_n_dev)
    arrived(es, fs.at[ci, xy, pl.ds(0, Z - 1)])
    es = exchange(lambda i: fs.at[ci, xy], fs.at[ci, xy], xy, XY, xy_dev)
    for zz in order:
        if zz < ZH:
            arrived(ph[zz], fb.at[zz, ci, xi, pl.ds(0, Y - 1)])
            own = fb.at[zz, ci, xi]
            ph[zz] = exchange(lambda i: own, own, xi, X, x_dev)
        else:
            arrived(ph[zz], fb.at[zz, ci, pl.ds(0, X - 1), yi])
            own = fb.at[zz, ci, :, yi]
            ph[zz] = exchange(lambda i: own, own, yi, Y, y_dev)
    arrived(es, fs.at[ci, pl.ds(0, XY - 1)])
    es = exchange(lambda i: fs.at[ci], fs.at[ci], ci, C, c_dev)
    arrived(es, fs.at[ci])
    row_mean = jnp.zeros((1, 128), F32)
    row_var = jnp.zeros((1, 128), F32)
    blocks = []
    for yy in range(Y):
        for zz in range(Z):
            for cc in range(C):
                b = fs[cc, yy, zz]
                for xx in range(1, X):
                    b = b + fs[cc, xx * Y + yy, zz]
                row_mean = row_mean + b[0:1]
                row_var = row_var + b[1:2]
                blocks.append(b[0:1])
    row_mean = row_mean / NDP
    for j in range(NDP):
        off = blocks[j] - row_mean
        row_var = row_var + W * (off * off)
        dm[j : j + 1] = off
    scale = to_cols((lax.rsqrt(row_var / D + EPS),))[:SEQ, 0:1]
    offs = jnp.transpose(dm[...])[:SEQ, :NDP]
    logits = jnp.dot(
        offs, gmat[...], preferred_element_type=F32, precision=lax.Precision.HIGHEST
    )

    def products(logits, zz):
        arrived(ph[zz], fb.at[zz, other])
        for yy in range(Y):
            lhs = jnp.concatenate(
                [
                    jnp.concatenate([fb[zz, cc, xx, yy] for xx in range(X)], axis=0)
                    for cc in range(C)
                ],
                axis=1,
            )
            b = (yy * Z + zz) * C * W
            logits = logits + lax.dot_general(
                lhs, emb[:, b : b + C * W], (((1,), (1,)), ((), ())), preferred_element_type=F32
            )
        return logits

    for n, zz in enumerate(order):
        if zz < ZH:
            arrived(ph[zz], fb.at[zz, ci, pl.ds(0, X - 1)])
        else:
            arrived(ph[zz], fb.at[zz, ci, :, pl.ds(0, Y - 1)])
        own = fb.at[zz, ci]
        ph[zz] = exchange(lambda i: own, own, ci, C, c_dev)
        if n > 0:
            logits = products(logits, order[n - 1])
    logits = products(logits, order[-1]) * scale

    top = jnp.max(logits, axis=1, keepdims=True)
    total = jnp.sum(jnp.exp(logits - top), axis=1, keepdims=True)

    def merged(buf):
        v = buf[...]
        tops, sums = v[:, 0:1], v[:, 1:2]
        best = jnp.max(tops, axis=0)
        return best, jnp.sum(sums * jnp.exp(tops - best[None]), axis=0)

    def joined(best, tot):
        r = lax.broadcasted_iota(jnp.int32, (2, 128), 0)
        return jnp.where(r == 0, best, tot)

    g1[xyc] = to_rows((top, total))[:2]
    eg = gather(g1, xyc, XY * C, xyc_dev)
    arrived(eg, g1.at[pl.ds(0, XY * C - 1)])
    g2[zz_own] = joined(*merged(g1))
    eg = gather(g2, zz_own, Z * H, zz_dev)
    arrived(eg, g2.at[pl.ds(0, Z * H - 1)])
    best, tot = merged(g2)
    stats = to_cols((best, jnp.log(tot)))[:SEQ]
    out_ref[...] = logits - stats[:, 0:1]
    lse_ref[...] = jnp.broadcast_to(stats[:, 1:2], (SEQ, V))
    for s, ref in pending:
        take(send_sem.at[s], ref)


def per_device(sizes, token_ids, cache_lengths, embedding, ln_gain, query_weight, key_cache,
               value_cache, out_weight, final_gain):
    Y, Z, C, X, H = sizes
    NDP, XY, ZH = Y * Z * C, X * Y, Z // 2
    V, D = embedding.shape
    SP, T, HW = key_cache.shape
    W = D // NDP
    SEQ = SP * NDP
    R = SEQ // X
    vmem = pl.BlockSpec(memory_space=pltpu.VMEM)
    smem = pl.BlockSpec(memory_space=pltpu.SMEM)
    hbm = pl.BlockSpec(memory_space=pl.ANY)
    logits, lse = pl.pallas_call(
        functools.partial(kernel, sizes),
        name="decode",
        out_shape=(
            jax.ShapeDtypeStruct((SEQ, V), F32),
            jax.ShapeDtypeStruct((SEQ, V), F32),
        ),
        in_specs=[vmem, smem, hbm, vmem, hbm, hbm, hbm, hbm, vmem],
        out_specs=(vmem, vmem),
        scratch_shapes=[
            pltpu.VMEM((V, D), BF16),
            pltpu.VMEM((W, HW), BF16),
            pltpu.VMEM((SP, T, HW), BF16),
            pltpu.VMEM((SP, T, HW), BF16),
            pltpu.VMEM((HW, W), BF16),
            pltpu.VMEM((C, Z, Y, X, R, W), BF16),
            pltpu.VMEM((Z, Y, X, R, W), BF16),
            pltpu.VMEM((ZH, X, Y, R, W), BF16),
            pltpu.VMEM((ZH, Y, R, W), BF16),
            pltpu.VMEM((ZH, Y, R, W), BF16),
            pltpu.VMEM((ZH, Y, X, R, W), BF16),
            pltpu.VMEM((ZH, X, R, W), BF16),
            pltpu.VMEM((ZH, X, R, W), BF16),
            pltpu.VMEM((Z, R, W), BF16),
            pltpu.VMEM((Z, R, W), BF16),
            pltpu.VMEM((H, R, W), BF16),
            pltpu.VMEM((X, R, W), BF16),
            pltpu.VMEM((C, 8, 128), F32),
            pltpu.VMEM((X, 8, 128), F32),
            pltpu.VMEM((Y, 8, 128), F32),
            pltpu.VMEM((Z, 8, 128), F32),
            pltpu.VMEM((H, 8, 128), F32),
            pltpu.VMEM((NDP, SP, HW), F32),
            pltpu.VMEM((NDP, SP, HW), F32),
            pltpu.VMEM((NDP, SP, HW), BF16),
            pltpu.VMEM((SEQ, HW), F32),
            pltpu.VMEM((X, R, W), F32),
            pltpu.VMEM((X, R, W), F32),
            pltpu.VMEM((H, R, W), BF16),
            pltpu.VMEM((NDP, V), F32),
            pltpu.VMEM((max(NDP, 128), 128), F32),
            pltpu.VMEM((Z, C, X, Y, R, W), BF16),
            pltpu.VMEM((C, XY, Z, 2, 128), F32),
            pltpu.VMEM((XY * C, 2, 128), F32),
            pltpu.VMEM((Z * H, 2, 128), F32),
            pltpu.SemaphoreType.DMA((Y + 4,)),
            pltpu.SemaphoreType.DMA((NSEM,)),
            pltpu.SemaphoreType.DMA((NSEM,)),
            pltpu.SemaphoreType.REGULAR((5,)),
        ],
        compiler_params=pltpu.CompilerParams(collective_id=0, has_side_effects=True),
    )(
        token_ids.reshape(1, -1), cache_lengths, embedding, ln_gain.reshape(1, -1), query_weight,
        key_cache, value_cache, out_weight, final_gain.reshape(1, -1),
    )
    return logits - lse


def solution(mesh, sizes=(4, 4, 2, 4, 4)):
    finer = Mesh(mesh.devices.reshape(sizes), DP_MP)
    placed = (
        P(),
        P(DP),
        P(DP_MP, None),
        P(),
        P(DP, MP),
        P(DP, None, MP),
        P(DP, None, MP),
        P(MP, DP),
        P(),
    )
    return jax.shard_map(
        functools.partial(per_device, sizes), mesh=finer, in_specs=placed,
        out_specs=P(None, DP_MP), check_vma=False,
    )
```

```python
import functools

import jax
import jax.numpy as jnp
from jax import lax
from jax.experimental import pallas as pl
from jax.experimental.pallas import tpu as pltpu
from jax.sharding import Mesh
from jax.sharding import PartitionSpec as P

HD = 128
EPS = 1e-5
DP_MP = ("dp_0", "dp_1", "dp_2", "mp_0", "mp_1")
DP = ("dp_0", "dp_1", "dp_2")
MP = ("mp_0", "mp_1")
MESH = pl.DeviceIdType.MESH
F32 = jnp.float32
BF16 = jnp.bfloat16
NSEM = 56


def kernel(
    sizes,
    ids_ref, len_ref, emb_ref, lng_ref, wq_ref, key_ref, val_ref, wo_ref, fg_ref,
    out_ref, lse_ref,
    emb, wq, key, val, wo,
    p, r1, a1, a2, a3, b1, b2, b3, t0, r3, r4, r5, s1, sx, sy, s3, s4,
    part, rq, mine, ra, att_all, ro2, gmat, dm, fb, fs, g1, g2,
    load_sem, send_sem, recv_sem, ring_sem,
):
    Y, Z, C, X, H = sizes
    NDP, XY, ZC, ZH = Y * Z * C, X * Y, Z * C, Z // 2
    V, D = emb.shape
    SP, T, HW = key.shape
    W = D // NDP
    SEQ = SP * NDP
    R = SEQ // X
    NH = HW // HD

    yi, zi, ci, xi, hi = (lax.axis_index(a) for a in DP_MP)
    xy = xi * Y + yi
    zz_own = hi * Z + zi
    xyc = xy * C + ci
    zc = zi * C + ci
    dp = (yi * Z + zi) * C + ci

    def xy_dev(i):
        return {"mp_0": lax.div(i, Y), "dp_0": lax.rem(i, Y)}

    def xyc_dev(i):
        return {"dp_2": lax.rem(i, C), **xy_dev(lax.div(i, C))}

    def zz_dev(i):
        return {"mp_1": lax.div(i, Z), "dp_1": lax.rem(i, Z)}

    def dp_dev(i):
        return {"dp_0": lax.div(i, ZC), "dp_1": lax.rem(lax.div(i, C), Z), "dp_2": lax.rem(i, C)}

    def y_dev(i):
        return {"dp_0": i}

    def z_dev(i):
        return {"dp_1": i}

    def c_dev(i):
        return {"dp_2": i}

    def x_dev(i):
        return {"mp_0": i}

    def h_dev(i):
        return {"mp_1": i}

    def each(n, body):
        if n <= 4:
            for k in range(1, n):
                body(k)
        else:
            lax.fori_loop(1, n, lambda k, _: body(k), None)

    def send(s, src, dst, dev):
        pltpu.make_async_remote_copy(
            src_ref=src, dst_ref=dst, send_sem=send_sem.at[s], recv_sem=recv_sem.at[s],
            device_id=dev, device_id_type=MESH,
        ).start()

    def take(sem, ref):
        pltpu.make_async_copy(ref, ref, sem).wait()

    pending = []
    used = [0]

    def new():
        used[0] += 1
        return used[0] - 1

    def arrived(s, ref):
        take(recv_sem.at[s], ref)
        pending.append((s, ref))

    def exchange(src, dst, own, n, dev):
        s = new()

        def body(k):
            i = lax.rem(own + k, n)
            send(s, src(i), dst, dev(i))

        each(n, body)
        return s

    def gather(buf, own, n, dev):
        return exchange(lambda i: buf.at[own], buf.at[own], own, n, dev)

    def to_rows(cols, start=None):
        n = cols[0].shape[0]
        lane = lax.broadcasted_iota(jnp.int32, (n, 128), 1)
        x = jnp.zeros((n, 128), F32)
        for k, col in enumerate(cols):
            x = jnp.where(lane == k, col, x)
        if start is not None:
            x = jnp.concatenate([x] * (SEQ // n), axis=0)
            r = lax.broadcasted_iota(jnp.int32, (SEQ, 128), 0)
            x = jnp.where((r >= start) & (r < start + n), x, 0.0)
        if x.shape[0] < 128:
            x = jnp.concatenate([x, jnp.zeros((128 - x.shape[0], 128), F32)], axis=0)
        return jnp.transpose(x)

    def to_cols(rows):
        row = lax.broadcasted_iota(jnp.int32, (128, 128), 0)
        x = jnp.zeros((128, 128), F32)
        for k, r in enumerate(rows):
            x = jnp.where(row == k, r, x)
        return jnp.transpose(x)

    wide = Z * C * W
    pairs = [
        (emb_ref.at[:, pl.ds(k * wide, wide)], emb.at[:, pl.ds(k * wide, wide)]) for k in range(Y)
    ]
    pairs += [(wq_ref, wq), (key_ref, key), (val_ref, val), (wo_ref, wo.at[xi])]
    loads = [pltpu.make_async_copy(a, b, load_sem.at[k]) for k, (a, b) in enumerate(pairs)]
    for c in loads:
        c.start()

    barrier = pltpu.get_barrier_semaphore()

    def greet(dev):
        pl.semaphore_signal(barrier, inc=1, device_id=dev, device_id_type=MESH)

    ring = Z * H
    greet(c_dev(1 - ci))
    for own, n, dev in ((xi, X, x_dev), (yi, Y, y_dev), (zi, Z, z_dev)):
        for k in range(1, n):
            greet(dev(lax.rem(own + k, n)))
    for k in (1, ring - 1):
        greet(zz_dev(lax.rem(zz_own + k, ring)))
    greeted = X + Y + Z
    rounds = [d for d in (1, 2, 4, 8, 16) if 2 * d < ring]

    def tell(r):
        if r < len(rounds):
            for k in (rounds[r], ring - rounds[r]):
                pl.semaphore_signal(
                    ring_sem.at[r], inc=1, device_id=zz_dev(lax.rem(zz_own + k, ring)),
                    device_id_type=MESH,
                )

    def told(r):
        if r < len(rounds):
            pl.semaphore_wait(ring_sem.at[r], 2)

    flat = (dp * X + xi) * H + hi
    ids = ids_ref[...]
    if SEQ < 128:
        ids = jnp.concatenate([ids, jnp.full((1, 128 - SEQ), -1, jnp.int32)], axis=1)
    row = lax.broadcasted_iota(jnp.int32, (128, 128), 0)
    hot = jnp.where((row + flat * V == ids) & (row < V), 1.0, 0.0).astype(F32)
    hot = jnp.transpose(hot)[:SEQ, :V].astype(BF16)

    other = 1 - ci
    acc = jnp.zeros((SEQ, 128), F32)
    order = [half * ZH + k for k in range(ZH) for half in (0, 1)]

    def rows_of(acc, core, zz, first):
        for yy in range(Y):
            if first:
                loads[yy].wait()
            b = (yy * Z + zz) * C + core
            cols = pl.ds(pl.multiple_of(b * W, 128), W)
            blk = jnp.dot(hot, emb[:, cols], preferred_element_type=F32)
            for j in range(0, W, 128):
                acc = acc + blk[:, j : j + 128]
            blk = blk.astype(BF16)
            for xx in range(X):
                p[core, zz, yy, xx] = blk[xx * R : (xx + 1) * R]
        return acc

    e1, ph = {}, {}
    for n, zz in enumerate(order):
        acc = rows_of(acc, other, zz, n == 0)
        if n == 0:
            pl.semaphore_wait(barrier, greeted)
        e1[zz] = new()
        send(e1[zz], p.at[other, zz], r1.at[zz], c_dev(other))
        if n == 0:
            tell(0)
    for n, zz in enumerate(order):
        acc = rows_of(acc, ci, zz, False)
        arrived(e1[zz], r1.at[zz])
        for yy in range(Y):
            for xx in range(X):
                r1[zz, yy, xx] = r1[zz, yy, xx] + p[ci, zz, yy, xx]
        if zz < ZH:
            ph[zz] = exchange(lambda i: r1.at[zz, :, i], a1.at[zz, xi], xi, X, x_dev)
            a1[zz, xi] = r1[zz, :, xi]
        else:
            ph[zz] = exchange(lambda i: r1.at[zz, i], b1.at[zz - ZH, yi], yi, Y, y_dev)
            b1[zz - ZH, yi] = r1[zz, yi]
        if n == 0:
            told(0)
            tell(1)

    mean = jnp.sum(acc, axis=1, keepdims=True) / D
    devs = []
    for xx in range(X):
        m = mean[xx * R : (xx + 1) * R]
        sq = jnp.zeros((R, 128), F32)
        for cc in range(C):
            for zz in range(Z):
                for yy in range(Y):
                    d = p[cc, zz, yy, xx].astype(F32) - m
                    for j in range(0, W, 128):
                        sq = sq + d[:, j : j + 128] * d[:, j : j + 128]
        devs.append(jnp.sum(sq, axis=1, keepdims=True) / D)
    var = jnp.concatenate(devs, axis=0)
    s1[ci] = to_rows((mean, var))[:8]
    es = gather(s1, ci, C, c_dev)
    told(1)
    tell(2)

    for n, zz in enumerate(order):
        if zz < ZH:
            arrived(ph[zz], a1.at[zz, pl.ds(0, X - 1)])
            for yy in range(Y):
                tot = a1[zz, 0, yy]
                for k in range(1, X):
                    tot = tot + a1[zz, k, yy]
                a2[zz, yy] = tot
            ph[zz] = exchange(lambda i: a2.at[zz, i], a3.at[zz, yi], yi, Y, y_dev)
            a3[zz, yi] = a2[zz, yi]
        else:
            k0 = zz - ZH
            arrived(ph[zz], b1.at[k0, pl.ds(0, Y - 1)])
            for xx in range(X):
                tot = b1[k0, 0, xx]
                for k in range(1, Y):
                    tot = tot + b1[k0, k, xx]
                b2[k0, xx] = tot
            ph[zz] = exchange(lambda i: b2.at[k0, i], b3.at[k0, xi], xi, X, x_dev)
            b3[k0, xi] = b2[k0, xi]
        if n == 0:
            arrived(es, s1.at[pl.ds(0, C - 1)])
            sx[xi] = jnp.sum(s1[...], axis=0)
            es = gather(sx, xi, X, x_dev)
    arrived(es, sx.at[pl.ds(0, X - 1)])
    sy[yi] = jnp.sum(sx[...], axis=0)
    es = gather(sy, yi, Y, y_dev)
    loads[Y + 3].wait()
    ew = new()

    def to_x(k):
        send(ew, wo.at[xi], wo.at[xi], x_dev(lax.rem(xi + k, X)))

    for k in range(1, X):
        if 2 * k != X:
            to_x(k)

    half_row = lax.broadcasted_iota(jnp.int32, (16, W), 0)
    for j in range(NDP):
        gain = fg_ref[:, j * W : (j + 1) * W]
        high = gain.astype(BF16).astype(F32)
        both = jnp.where(half_row == 0, high, jnp.where(half_row == 1, gain - high, 0.0))
        got = lax.dot_general(
            both.astype(BF16), emb[:, j * W : (j + 1) * W], (((1,), (1,)), ((), ())),
            preferred_element_type=F32,
        )
        gmat[j : j + 1] = got[0:1] + got[1:2]

    ez = new()
    for zz in order:
        if zz < ZH:
            buf, cnt, k0 = a3, Y, zz
        else:
            buf, cnt, k0 = b3, X, zz - ZH
        arrived(ph[zz], buf.at[k0, pl.ds(0, cnt - 1)])
        tot = buf[k0, 0]
        for k in range(1, cnt):
            tot = tot + buf[k0, k]
        t0[zz] = tot

        @pl.when(zi != zz)
        def _():
            send(ez, t0.at[zz], r3.at[zi], z_dev(jnp.int32(zz)))

    r3[zi] = t0[zi]
    arrived(es, sy.at[pl.ds(0, Y - 1)])
    s3[zi] = jnp.sum(sy[...], axis=0)
    es = gather(s3, zi, Z, z_dev)

    arrived(ez, r3.at[pl.ds(0, Z - 1)])
    tot = r3[0]
    for k in range(1, Z):
        tot = tot + r3[k]
    r4[hi] = tot
    told(2)
    if H > 1:
        ez = gather(r4, hi, H, h_dev)
    arrived(es, s3.at[pl.ds(0, Z - 1)])
    s4[hi] = jnp.sum(s3[...], axis=0)
    if H > 1:
        es = gather(s4, hi, H, h_dev)
        arrived(ez, r4.at[pl.ds(0, H - 1)])
    tot = r4[0]
    for k in range(1, H):
        tot = tot + r4[k]
    r5[xi] = tot
    ex = gather(r5, xi, X, x_dev)
    to_x(X // 2)
    if H > 1:
        arrived(es, s4.at[pl.ds(0, H - 1)])
    stats = jnp.sum(s4[...], axis=0)
    stats = to_cols((stats[0:1], stats[1:2]))
    mean, var = stats[:SEQ, 0:1], stats[:SEQ, 1:2]
    arrived(ex, r5.at[pl.ds(0, X - 1)])

    own_cols = pl.ds(pl.multiple_of(dp * W, 128), W)
    embedded = r5[...].reshape(SEQ, W).astype(F32)
    normed = (lng_ref[:, own_cols] * (embedded - mean) * lax.rsqrt(var + EPS)).astype(BF16)
    loads[Y].wait()
    partial = jnp.dot(normed, wq[...], preferred_element_type=F32)
    for j in range(NDP):
        part[j] = partial[j * SP : (j + 1) * SP]
    eq = exchange(lambda i: part.at[i], rq.at[dp], dp, NDP, dp_dev)
    rq[dp] = part[dp]
    loads[Y + 1].wait()
    loads[Y + 2].wait()
    arrived(eq, rq.at[pl.ds(0, NDP - 1)])
    queries = (jnp.sum(rq[...], axis=0) * HD**-0.5).astype(BF16).astype(F32)

    head = lax.broadcasted_iota(jnp.int32, (8, HW), 0) * HD
    lane = lax.broadcasted_iota(jnp.int32, (8, HW), 1)
    own_head = (lane >= head) & (lane < head + HD)
    place = lax.broadcasted_iota(jnp.int32, (8, T), 1)
    pair = lax.broadcasted_iota(jnp.int32, (SP, HW), 0)
    attended = jnp.zeros((SP, HW), F32)
    for s in range(SP):
        q = jnp.where(own_head, queries[s : s + 1], 0.0).astype(BF16)
        scores = lax.dot_general(
            q, key[s], (((1,), (1,)), ((), ())), preferred_element_type=F32
        )
        scores = jnp.where(place < len_ref[s], scores, -1e30)
        e = jnp.exp(scores - jnp.max(scores, axis=1, keepdims=True))
        w = (e / jnp.sum(e, axis=1, keepdims=True)).astype(BF16)
        got = jnp.dot(w, val[s], preferred_element_type=F32)
        got = jnp.sum(jnp.where(own_head, got, 0.0), axis=0, keepdims=True)
        attended = jnp.where(pair == s, got, attended)
    mine[...] = attended.astype(BF16)
    slot = xi * ZC + zc
    et = new()

    def to_quarter(i):
        send(et, mine, ra.at[slot], {**dp_dev(i), "mp_0": yi})

    each(NDP, lambda k: to_quarter(lax.rem(dp + k, NDP)))

    @pl.when(xi != yi)
    def _():
        to_quarter(dp)

    @pl.when(xi == yi)
    def _():
        ra[slot] = mine[...]

    def attended_waits(sem):
        @pl.when(xi != yi)
        def _():
            take(sem, ra)

        @pl.when(xi == yi)
        def _():
            take(sem, ra.at[pl.ds(0, X * ZC - 1)])

    arrived(ew, wo.at[pl.ds(0, X - 1)])
    attended_waits(recv_sem.at[et])
    for xx in range(X):
        for j in range(ZC):
            att_all[j * SP : (j + 1) * SP, xx * HW : (xx + 1) * HW] = ra[xx * ZC + j].astype(F32)
    mixed = jnp.dot(
        att_all[...].astype(BF16), wo[...].reshape(X * HW, W), preferred_element_type=F32
    )
    ro2[hi] = mixed.astype(BF16)
    if H > 1:
        eo = gather(ro2, hi, H, h_dev)
        arrived(eo, ro2.at[pl.ds(0, H - 1)])
    hidden = r5[xi].astype(F32) + jnp.sum(ro2[...].astype(F32), axis=0)

    m = jnp.sum(hidden, axis=1, keepdims=True) / W
    d = hidden - m
    fb[zi, ci, xi, yi] = (fg_ref[:, own_cols] * d).astype(BF16)
    ef = exchange(lambda i: fb.at[zi, ci, xi, yi], fb.at[zi, ci, xi, yi], zi, Z, z_dev)
    fs[ci, xy, zi] = to_rows((m, jnp.sum(d * d, axis=1, keepdims=True)), xi * R)[:2]
    es = exchange(lambda i: fs.at[ci, xy, zi], fs.at[ci, xy, zi], zi, Z, z_dev)

    arrived(ef, fb.at[pl.ds(0, Z - 1), 0, 0, 0])
    for zz in order:
        own = fb.at[zz, ci, xi, yi]
        own_n_dev = (yi, Y, y_dev) if zz < ZH else (xi, X, x_dev)
        ph[zz] = exchange(lambda i: own, own, *own_n_dev)
    arrived(es, fs.at[ci, xy, pl.ds(0, Z - 1)])
    es = exchange(lambda i: fs.at[ci, xy], fs.at[ci, xy], xy, XY, xy_dev)
    for zz in order:
        if zz < ZH:
            arrived(ph[zz], fb.at[zz, ci, xi, pl.ds(0, Y - 1)])
            own = fb.at[zz, ci, xi]
            ph[zz] = exchange(lambda i: own, own, xi, X, x_dev)
        else:
            arrived(ph[zz], fb.at[zz, ci, pl.ds(0, X - 1), yi])
            own = fb.at[zz, ci, :, yi]
            ph[zz] = exchange(lambda i: own, own, yi, Y, y_dev)
    arrived(es, fs.at[ci, pl.ds(0, XY - 1)])
    es = exchange(lambda i: fs.at[ci], fs.at[ci], ci, C, c_dev)
    arrived(es, fs.at[ci])
    row_mean = jnp.zeros((1, 128), F32)
    row_var = jnp.zeros((1, 128), F32)
    blocks = []
    for yy in range(Y):
        for zz in range(Z):
            for cc in range(C):
                b = fs[cc, yy, zz]
                for xx in range(1, X):
                    b = b + fs[cc, xx * Y + yy, zz]
                row_mean = row_mean + b[0:1]
                row_var = row_var + b[1:2]
                blocks.append(b[0:1])
    row_mean = row_mean / NDP
    for j in range(NDP):
        off = blocks[j] - row_mean
        row_var = row_var + W * (off * off)
        dm[j : j + 1] = off
    scale = to_cols((lax.rsqrt(row_var / D + EPS),))[:SEQ, 0:1]
    offs = jnp.transpose(dm[...])[:SEQ, :NDP]
    logits = jnp.dot(
        offs, gmat[...], preferred_element_type=F32, precision=lax.Precision.HIGHEST
    )

    def products(logits, zz):
        arrived(ph[zz], fb.at[zz, other])
        for yy in range(Y):
            lhs = jnp.concatenate(
                [
                    jnp.concatenate([fb[zz, cc, xx, yy] for xx in range(X)], axis=0)
                    for cc in range(C)
                ],
                axis=1,
            )
            b = (yy * Z + zz) * C * W
            logits = logits + lax.dot_general(
                lhs, emb[:, b : b + C * W], (((1,), (1,)), ((), ())), preferred_element_type=F32
            )
        return logits

    for n, zz in enumerate(order):
        if zz < ZH:
            arrived(ph[zz], fb.at[zz, ci, pl.ds(0, X - 1)])
        else:
            arrived(ph[zz], fb.at[zz, ci, :, pl.ds(0, Y - 1)])
        own = fb.at[zz, ci]
        ph[zz] = exchange(lambda i: own, own, ci, C, c_dev)
        if n > 0:
            logits = products(logits, order[n - 1])
    logits = products(logits, order[-1]) * scale

    top = jnp.max(logits, axis=1, keepdims=True)
    total = jnp.sum(jnp.exp(logits - top), axis=1, keepdims=True)

    def merged(buf):
        v = buf[...]
        tops, sums = v[:, 0:1], v[:, 1:2]
        best = jnp.max(tops, axis=0)
        return best, jnp.sum(sums * jnp.exp(tops - best[None]), axis=0)

    def joined(best, tot):
        r = lax.broadcasted_iota(jnp.int32, (2, 128), 0)
        return jnp.where(r == 0, best, tot)

    g1[xyc] = to_rows((top, total))[:2]
    eg = gather(g1, xyc, XY * C, xyc_dev)
    arrived(eg, g1.at[pl.ds(0, XY * C - 1)])
    g2[zz_own] = joined(*merged(g1))
    eg = gather(g2, zz_own, Z * H, zz_dev)
    arrived(eg, g2.at[pl.ds(0, Z * H - 1)])
    best, tot = merged(g2)
    stats = to_cols((best, jnp.log(tot)))[:SEQ]
    out_ref[...] = logits - stats[:, 0:1]
    lse_ref[...] = jnp.broadcast_to(stats[:, 1:2], (SEQ, V))
    attended_waits(send_sem.at[et])
    for s, ref in pending:
        take(send_sem.at[s], ref)


def per_device(sizes, token_ids, cache_lengths, embedding, ln_gain, query_weight, key_cache,
               value_cache, out_weight, final_gain):
    Y, Z, C, X, H = sizes
    NDP, XY, ZH = Y * Z * C, X * Y, Z // 2
    V, D = embedding.shape
    SP, T, HW = key_cache.shape
    W = D // NDP
    SEQ = SP * NDP
    R = SEQ // X
    vmem = pl.BlockSpec(memory_space=pltpu.VMEM)
    smem = pl.BlockSpec(memory_space=pltpu.SMEM)
    hbm = pl.BlockSpec(memory_space=pl.ANY)
    logits, lse = pl.pallas_call(
        functools.partial(kernel, sizes),
        name="decode",
        out_shape=(
            jax.ShapeDtypeStruct((SEQ, V), F32),
            jax.ShapeDtypeStruct((SEQ, V), F32),
        ),
        in_specs=[vmem, smem, hbm, vmem, hbm, hbm, hbm, hbm, vmem],
        out_specs=(vmem, vmem),
        scratch_shapes=[
            pltpu.VMEM((V, D), BF16),
            pltpu.VMEM((W, HW), BF16),
            pltpu.VMEM((SP, T, HW), BF16),
            pltpu.VMEM((SP, T, HW), BF16),
            pltpu.VMEM((X, HW, W), BF16),
            pltpu.VMEM((C, Z, Y, X, R, W), BF16),
            pltpu.VMEM((Z, Y, X, R, W), BF16),
            pltpu.VMEM((ZH, X, Y, R, W), BF16),
            pltpu.VMEM((ZH, Y, R, W), BF16),
            pltpu.VMEM((ZH, Y, R, W), BF16),
            pltpu.VMEM((ZH, Y, X, R, W), BF16),
            pltpu.VMEM((ZH, X, R, W), BF16),
            pltpu.VMEM((ZH, X, R, W), BF16),
            pltpu.VMEM((Z, R, W), BF16),
            pltpu.VMEM((Z, R, W), BF16),
            pltpu.VMEM((H, R, W), BF16),
            pltpu.VMEM((X, R, W), BF16),
            pltpu.VMEM((C, 8, 128), F32),
            pltpu.VMEM((X, 8, 128), F32),
            pltpu.VMEM((Y, 8, 128), F32),
            pltpu.VMEM((Z, 8, 128), F32),
            pltpu.VMEM((H, 8, 128), F32),
            pltpu.VMEM((NDP, SP, HW), F32),
            pltpu.VMEM((NDP, SP, HW), F32),
            pltpu.VMEM((SP, HW), BF16),
            pltpu.VMEM((X * Z * C, SP, HW), BF16),
            pltpu.VMEM((R, X * HW), F32),
            pltpu.VMEM((H, R, W), BF16),
            pltpu.VMEM((NDP, V), F32),
            pltpu.VMEM((max(NDP, 128), 128), F32),
            pltpu.VMEM((Z, C, X, Y, R, W), BF16),
            pltpu.VMEM((C, XY, Z, 2, 128), F32),
            pltpu.VMEM((XY * C, 2, 128), F32),
            pltpu.VMEM((Z * H, 2, 128), F32),
            pltpu.SemaphoreType.DMA((Y + 4,)),
            pltpu.SemaphoreType.DMA((NSEM,)),
            pltpu.SemaphoreType.DMA((NSEM,)),
            pltpu.SemaphoreType.REGULAR((5,)),
        ],
        compiler_params=pltpu.CompilerParams(collective_id=0, has_side_effects=True),
    )(
        token_ids.reshape(1, -1), cache_lengths, embedding, ln_gain.reshape(1, -1), query_weight,
        key_cache, value_cache, out_weight, final_gain.reshape(1, -1),
    )
    return logits - lse


def solution(mesh, sizes=(4, 4, 2, 4, 4)):
    finer = Mesh(mesh.devices.reshape(sizes), DP_MP)
    placed = (
        P(),
        P(DP),
        P(DP_MP, None),
        P(),
        P(DP, MP),
        P(DP, None, MP),
        P(DP, None, MP),
        P(MP, DP),
        P(),
    )
    return jax.shard_map(
        functools.partial(per_device, sizes), mesh=finer, in_specs=placed,
        out_specs=P(None, DP_MP), check_vma=False,
    )
```
